256 devices in a mesh: dap: 16 (over x, z_lo), cplx: 16 (over y, z_hi, core).
Axes of the slice: x: 4, y: 4, z: 8 (z_hi: 2, z_lo: 4; z = z_hi * 4 + z_lo), core: 2. Of those that a mesh axis runs over, the one named last changes fastest.
Arguments:
- pair: bfloat16 [192, 3072, 128], P('dap', 'cplx'), parts along dimension 1, may hold values from -6 to 6
- cotangent: bfloat16 [192, 3072, 128], P('dap', 'cplx'), parts along dimension 1, may hold values from -6 to 6
- residue_mask: int32 [3072], P('cplx'), parts along dimension 0, may hold values 0 or 1
- chain_ids: int32 [3072], P('cplx'), parts along dimension 0, may hold values from 0 to 2, never falling along the last dimension, each value on 1 to 96 neighbouring positions
- chain_embed: float32 [2, 128], replicated, may hold values from -4 to 4
- out_norm_gain: float32 [128], replicated, may hold values from 0.25 to 1.75
- out_proj: bfloat16 [128, 512], replicated, may hold values from -0.5 to 0.5
- out_gate: bfloat16 [128, 128], replicated, may hold values from -0.5 to 0.5
- out_mid_gain: float32 [128], replicated, may hold values from 0.25 to 1.75
- out_final: bfloat16 [128, 128], replicated, may hold values from -0.5 to 0.5
- in_norm_gain: float32 [128], replicated, may hold values from 0.25 to 1.75
- in_proj: bfloat16 [128, 512], replicated, may hold values from -0.5 to 0.5
- in_gate: bfloat16 [128, 128], replicated, may hold values from -0.5 to 0.5
- in_mid_gain: float32 [128], replicated, may hold values from 0.25 to 1.75
- in_final: bfloat16 [128, 128], replicated, may hold values from -0.5 to 0.5
Outputs:
- pair_grad: bfloat16 [192, 3072, 128], P('dap', 'cplx'), parts along dimension 1
- grad_proj: float32 [2048, 512], P('cplx'), parts along dimension 0
- grad_gate: float32 [2048, 128], P('cplx'), parts along dimension 0
- grad_final: float32 [2048, 128], P('cplx'), parts along dimension 0
- grad_norm_gain: float32 [2048], P('cplx'), parts along dimension 0
- grad_mid_gain: float32 [2048], P('cplx'), parts along dimension 0
The draws below stay inside these ranges and needn't reach their ends.
There are 16 independent parts, one for each index of `cplx`. The reference program is written for one: setup_inputs(seed, part) draws one part's arguments, and reference() takes and returns one part's arrays. A program takes and returns all parts, laid end to end along the dimension named above; an argument that names none is the same for every part. Nothing has to cross between parts.
Inputs may be any that keep to these rules, and one draw needn't show every extreme that they name: `chain_ids`: chain numbers never fall along the residues; each chain has at most 96 residues.
All inputs are finite; a program needn't handle non-finite values.
Results may differ from the reference program's by a relative error of at most 0.019.
Values may be sent and summed in bfloat16 or wider, within the bound.
A program may use at most 128 MiB of HBM per device.

```python
import math
import jax
import jax.numpy as jnp
import numpy as np
from jax import lax

C = 128
HID = 128
N_RES = 192


def plant(result, rng, smallest, high):
    place = [jax.random.randint(jax.random.fold_in(rng, axis), (), 0, length) for axis, length in enumerate(result.shape)]
    widest = result.shape.index(max(result.shape))
    neighbour = place[:widest] + [(place[widest] + 1) % result.shape[widest]] + place[widest + 1:]
    return result.at[tuple(place)].set(smallest).at[tuple(neighbour)].set(high)


def shard_levels(key, extent, cuts, least, high):
    factor_of = 1.0
    for position, blocks in cuts:
        draws = jax.random.uniform(jax.random.fold_in(jax.random.fold_in(key, 6), position), (blocks,), jnp.float32, least / len(cuts), high / len(cuts))
        factor_of = factor_of * jnp.repeat(jnp.exp(draws), extent[position] // blocks).reshape((-1,) + (1,) * (len(extent) - 1 - position))
    return factor_of


def split_up(number_of, total, most, skew):
    loads = [(1 << 20) // math.isqrt(rank ** skew) + 1 for rank in range(2, number_of + 1)]
    surplus, counts = total - most - (number_of - 1), [1] * (number_of - 1)
    while surplus > 0:
        free = [i for i in range(number_of - 1) if counts[i] < most]
        pool, left = sum([loads[i] for i in free]), surplus
        for i in free:
            addition = min(most - counts[i], max(1, left * loads[i] // pool), surplus)
            counts[i] = counts[i] + addition
            surplus = surplus - addition
    return np.array([most] + counts)


def uneven_parts(rng, amount, total, limit, skew):
    if amount == 2:
        one = jax.random.randint(rng, (), max(1, total - limit), min(limit, total - 1) + 1)
        return jnp.stack([one, total - one])
    tallies = jnp.asarray(split_up(amount, total, limit, skew), jnp.int32)
    twos = (amount - 1) // 2
    donor, sink = tallies[1:1 + 2 * twos:2], tallies[2:2 + 2 * twos:2]
    margin = jnp.minimum(donor - 1, limit - sink)
    shifted = jax.random.randint(jax.random.fold_in(rng, 1), (twos,), 0, 1 << 20) % (margin + 1)
    tallies = tallies.at[1:1 + 2 * twos:2].set(donor - shifted).at[2:2 + 2 * twos:2].set(sink + shifted)
    return tallies[jax.random.permutation(jax.random.fold_in(rng, 2), amount)]


def normal_values(stream_key, dims, deviation, most, cuts=(), dtype=jnp.bfloat16):
    drawn = jax.random.normal(stream_key, dims, jnp.float32) * deviation
    if len(cuts) > 0:
        drawn = shard_levels(stream_key, dims, cuts, -0.22, 0.18) * drawn
    return jnp.clip(drawn, min=-most, max=most).astype(dtype)


def setup_inputs(seed: int = 0, part: int = 0) -> dict:
    arg_keys = jax.random.split(jax.random.key(seed), 16)
    part_splits = jax.random.split(jax.random.fold_in(arg_keys[15], part), 16)
    return {
        "pair": normal_values(part_splits[0], (N_RES, N_RES, C), 1.0, 6.0, ((0, 16),)),
        "cotangent": normal_values(part_splits[1], (N_RES, N_RES, C), 1.0, 6.0, ((0, 16),)),
        "residue_mask": plant((jax.random.randint(part_splits[2], (N_RES,), 0, 8) < 7).astype(jnp.int32), jax.random.fold_in(part_splits[2], 1), 0, 1),
        "chain_ids": jnp.searchsorted(jnp.cumsum(uneven_parts(part_splits[3], 3, N_RES, N_RES // 2, 0)), jnp.arange(N_RES), side="right").astype(jnp.int32),
        "chain_embed": normal_values(arg_keys[4], (2, C), 1.0, 4.0, (), jnp.float32),
        "out_norm_gain": jnp.clip(1.0 + 0.15 * jax.random.normal(arg_keys[5], (C,), jnp.float32), 0.25, 1.75),
        "out_proj": normal_values(arg_keys[6], (C, 4 * HID), C ** -0.5, 0.5),
        "out_gate": normal_values(arg_keys[7], (C, C), C ** -0.5, 0.5),
        "out_mid_gain": jnp.clip(1.0 + 0.15 * jax.random.normal(arg_keys[8], (HID,), jnp.float32), 0.25, 1.75),
        "out_final": normal_values(arg_keys[9], (HID, C), HID ** -0.5, 0.5),
        "in_norm_gain": jnp.clip(1.0 + 0.15 * jax.random.normal(arg_keys[10], (C,), jnp.float32), 0.25, 1.75),
        "in_proj": normal_values(arg_keys[11], (C, 4 * HID), C ** -0.5, 0.5),
        "in_gate": normal_values(arg_keys[12], (C, C), C ** -0.5, 0.5),
        "in_mid_gain": jnp.clip(1.0 + 0.15 * jax.random.normal(arg_keys[13], (HID,), jnp.float32), 0.25, 1.75),
        "in_final": normal_values(arg_keys[14], (HID, C), HID ** -0.5, 0.5),
    }


def layer_norm(values_in, gain):
    average = lax.optimization_barrier(jnp.mean(values_in, axis=-1, keepdims=True))
    centred = values_in - average
    variance = lax.optimization_barrier(jnp.mean(centred * centred, axis=-1, keepdims=True))
    return centred * jax.lax.rsqrt(variance + 1e-05) * gain

def gated_pair(projected, pair_mask, hidden_width):
    masked = pair_mask[..., None]
    left_act = masked * jax.nn.sigmoid(projected[..., :hidden_width]) * projected[..., hidden_width:2 * hidden_width]
    right_act = masked * jax.nn.sigmoid(projected[..., 2 * hidden_width:3 * hidden_width]) * projected[..., 3 * hidden_width:]
    return (left_act, right_act)

def reference(pair, cotangent, residue_mask, chain_ids, chain_embed, out_norm_gain, out_proj, out_gate, out_mid_gain, out_final, in_norm_gain, in_proj, in_gate, in_mid_gain, in_final):
    f32 = jnp.float32
    bf16 = jnp.bfloat16
    hidden_width = out_final.shape[0]
    res_count = pair.shape[0]
    inv_count = 1.0 / res_count
    pair_mask = (residue_mask[:, None] * residue_mask[None, :]).astype(f32)
    same_chain = chain_ids[:, None] == chain_ids[None, :]
    start = pair.astype(f32) + jnp.where(same_chain[..., None], chain_embed[1], chain_embed[0])
    out_normed = layer_norm(start, out_norm_gain).astype(bf16)
    projected = jnp.dot(out_normed, out_proj, preferred_element_type=f32)
    left_act, right_act = gated_pair(projected, pair_mask, hidden_width)
    left_b = left_act.astype(bf16)
    right_b = right_act.astype(bf16)
    x_out = jnp.einsum('ikc,jkc->ijc', left_b.astype(f32), right_b.astype(f32))
    y_out = layer_norm(x_out, out_mid_gain).astype(bf16)
    update = jax.nn.sigmoid(jnp.dot(out_normed, out_gate, preferred_element_type=f32)) * jnp.dot(y_out, out_final, preferred_element_type=f32)
    pair_mid = (start + update).astype(bf16)
    mid_f32 = pair_mid.astype(f32)
    normed_f32, norm_back = jax.vjp(layer_norm, mid_f32, in_norm_gain)
    in_normed = normed_f32.astype(bf16)
    proj_in = jnp.dot(in_normed, in_proj, preferred_element_type=f32)
    (left_in, right_in), glu_back = jax.vjp(lambda proj_val: gated_pair(proj_val, pair_mask, hidden_width), proj_in)
    left_ib = left_in.astype(bf16)
    right_ib = right_in.astype(bf16)
    x_in = jnp.einsum('kic,kjc->ijc', left_ib.astype(f32), right_ib.astype(f32))
    y_f32, mid_back = jax.vjp(layer_norm, x_in, in_mid_gain)
    y_in = y_f32.astype(bf16)
    logit = jnp.dot(in_normed, in_gate, preferred_element_type=f32)
    value = jnp.dot(y_in, in_final, preferred_element_type=f32)
    sigma = jax.nn.sigmoid(logit)
    upstream = cotangent.astype(f32)
    grad_value = (upstream * sigma).astype(bf16)
    grad_logit = (upstream * value * sigma * (1.0 - sigma)).astype(bf16)
    grad_final = jnp.einsum('ijc,ijd->cd', y_in.astype(f32), grad_value.astype(f32)) * inv_count
    grad_gate = jnp.einsum('ijc,ijd->cd', in_normed.astype(f32), grad_logit.astype(f32)) * inv_count
    grad_y = jnp.dot(grad_value, in_final.T, preferred_element_type=f32)
    grad_x, grad_mid = mid_back(grad_y)
    grad_x_b = grad_x.astype(bf16).astype(f32)
    grad_a = jnp.einsum('kjc,ijc->kic', right_ib.astype(f32), grad_x_b)
    grad_b = jnp.einsum('kic,ijc->kjc', left_ib.astype(f32), grad_x_b)
    grad_p = glu_back((grad_a, grad_b))[0].astype(bf16)
    grad_proj = jnp.einsum('ijc,ijd->cd', in_normed.astype(f32), grad_p.astype(f32)) * inv_count
    grad_normed = jnp.dot(grad_p, in_proj.T, preferred_element_type=f32) + jnp.dot(grad_logit, in_gate.T, preferred_element_type=f32)
    grad_z, grad_norm = norm_back(grad_normed)
    pair_grad = (upstream + grad_z).astype(bf16)
    return (pair_grad, grad_proj, grad_gate, grad_final, grad_norm * inv_count, grad_mid * inv_count)
```

```python
import functools

import jax
import jax.numpy as jnp
from jax import lax
from jax.experimental import pallas as pl
from jax.experimental.pallas import tpu as pltpu
from jax.sharding import PartitionSpec as P

f32 = jnp.float32
bf16 = jnp.bfloat16

ROWS, RES, CH, DEV = 12, 192, 128, 16
CG = CH // DEV
STEPS = ROWS // 2
W = 2 * RES
PAIRS = ROWS * RES
HALF = PAIRS // 2
EPS = 1e-5
INV = 1.0 / RES
VM = pl.BlockSpec(memory_space=pltpu.VMEM)
LIMIT = 60 * 1024 * 1024


def dot(a, b, ca, cb):
    return lax.dot_general(a, b, (((ca,), (cb,)), ((), ())), preferred_element_type=f32)


def lanes_of(m, width=W):
    return pl.ds(pl.multiple_of(m * width, 128), width)


def norm_stats(v):
    mean = jnp.mean(v, axis=0, keepdims=True)
    cent = v - mean
    var = jnp.mean(cent * cent, axis=0, keepdims=True)
    rstd = lax.rsqrt(var + EPS)
    return cent * rstd, rstd


def sig(v):
    return jax.nn.sigmoid(v)


def to_channels(pair_ref, sel, m):
    two = pair_ref[pl.ds(2 * m, 2)].reshape(W, CH)
    return dot(two, sel, 0, 0)


def pre_kernel(pair_ref, sel_ref, rows_ref, vec_ref, w_ref, start_ref, gate_ref, ab_ref):
    def step(m, _):
        at = lanes_of(m)
        st = to_channels(pair_ref, sel_ref[...], m)
        same = rows_ref[1:2, at]
        st = st + jnp.where(same > 0.5, vec_ref[:, 1:2], vec_ref[:, 0:1])
        start_ref[:, at] = st
        xhat, _ = norm_stats(st)
        normed = (xhat * vec_ref[:, 2:3]).astype(bf16)
        p = dot(w_ref[...], normed, 1, 0)
        pm = rows_ref[0:1, at]
        ab = pm * sig(p[0:256]) * p[256:512]
        ab_ref[:, :, at] = ab.astype(bf16).reshape(DEV, 16, W)
        gate_ref[:, at] = sig(p[512:640])
        return 0

    lax.fori_loop(0, STEPS, step, 0)


def load_x(x_ref, m3):
    at = lanes_of(m3)
    both = x_ref[:, :, at].astype(f32)
    return [both[:, 8 * h : 8 * h + 8].reshape(CH, W) for h in (0, 1)]


def mid_kernel(x_ref, start_ref, gate_ref, rows_ref, vec_ref, wf_ref, w_ref, mid_ref, nrm_ref, ab_ref):
    def step(m3, _):
        for h, x in enumerate(load_x(x_ref, m3)):
            at = lanes_of(m3 + 3 * h)
            xhat, _ = norm_stats(x)
            y = (xhat * vec_ref[:, 3:4]).astype(bf16)
            upd = gate_ref[:, at] * dot(wf_ref[...], y, 1, 0)
            mid = (start_ref[:, at] + upd).astype(bf16)
            mid_ref[:, at] = mid
            zhat, _ = norm_stats(mid.astype(f32))
            normed = (zhat * vec_ref[:, 4:5]).astype(bf16)
            nrm_ref[:, at] = normed
            p = dot(w_ref[...], normed, 1, 0)
            ab = rows_ref[0:1, at] * sig(p[0:256]) * p[256:512]
            ab_ref[:, :, at] = ab.astype(bf16).reshape(DEV, 16, W)
        return 0

    lax.fori_loop(0, 3, step, 0)


def lane_sum(v):
    total = v[:, 0:128]
    for t in range(1, v.shape[1] // 128):
        total = total + v[:, 128 * t : 128 * t + 128]
    return total


def value_kernel(
    x_ref, ct_ref, nrm_ref, sel_ref, vec_ref, wgt_ref, wft_ref, wf_ref,
    gx_ref, gl_ref, ggate_ref, gfinal_ref, gmid_ref,
):
    ggate_ref[...] = jnp.zeros_like(ggate_ref)
    gfinal_ref[...] = jnp.zeros_like(gfinal_ref)
    gmid_ref[...] = jnp.zeros_like(gmid_ref)

    def step(m3, _):
        grads = []
        for h, x in enumerate(load_x(x_ref, m3)):
            m = m3 + 3 * h
            at = lanes_of(m)
            xhat, rstd = norm_stats(x)
            gain = vec_ref[:, 5:6]
            y = (xhat * gain).astype(bf16)
            normed = nrm_ref[:, at]
            ct = to_channels(ct_ref, sel_ref[...], m)
            s = sig(dot(wgt_ref[...], normed, 1, 0))
            value = dot(wft_ref[...], y, 1, 0)
            gv = (ct * s).astype(bf16)
            gl = (ct * value * s * (1.0 - s)).astype(bf16)
            gl_ref[:, at] = gl
            gfinal_ref[...] += dot(y, gv, 1, 1)
            ggate_ref[...] += dot(normed, gl, 1, 1)
            gy = dot(wf_ref[...], gv, 1, 0)
            gmid_ref[...] += lane_sum(gy * xhat)
            gh = gy * gain
            gx = rstd * (
                gh
                - jnp.mean(gh, axis=0, keepdims=True)
                - xhat * jnp.mean(gh * xhat, axis=0, keepdims=True)
            )
            grads.append(gx.reshape(DEV, CG, W))
        gx_ref[:, :, lanes_of(m3)] = jnp.concatenate(grads, axis=1).astype(bf16)
        return 0

    lax.fori_loop(0, 3, step, 0)


def post_kernel(
    gab_ref, ct_ref, mid_ref, nrm_ref, gl_ref, sel_ref, rows_ref, vec_ref, w_ref, wt_ref, wg_ref,
    out_ref, gproj_ref, gnorm_ref,
):
    gproj_ref[...] = jnp.zeros_like(gproj_ref)
    gnorm_ref[...] = jnp.zeros_like(gnorm_ref)

    def step(m, _):
        at = lanes_of(m)
        normed = nrm_ref[:, at]
        p = dot(w_ref[...], normed, 1, 0)
        g = sig(p[0:256])
        v = p[256:512]
        gab = gab_ref[:, :, at].reshape(256, W).astype(f32) * rows_ref[0:1, at]
        gp = jnp.concatenate([gab * v * g * (1.0 - g), gab * g], axis=0).astype(bf16)
        gproj_ref[...] += dot(gp, normed, 1, 1)
        gn = dot(wt_ref[...], gp, 1, 0) + dot(wg_ref[...], gl_ref[:, at], 1, 0)
        zhat, rstd = norm_stats(mid_ref[:, at].astype(f32))
        gnorm_ref[...] += lane_sum(gn * zhat)
        gh = gn * vec_ref[:, 4:5]
        gz = rstd * (
            gh
            - jnp.mean(gh, axis=0, keepdims=True)
            - zhat * jnp.mean(gh * zhat, axis=0, keepdims=True)
        )
        ct = to_channels(ct_ref, sel_ref[...], m)
        res = (ct + gz).astype(bf16)
        back = dot(sel_ref[...], res, 1, 1)
        out_ref[pl.ds(2 * m, 2)] = back.astype(bf16).reshape(2, RES, CH)
        return 0

    lax.fori_loop(0, STEPS, step, 0)


def peers():
    me = lax.axis_index("dap")
    mx, mz = me // 4, me % 4
    out = []
    for dz in (2, 3, 1, 0):
        for dx in range(4):
            if dx == 0 and dz == 0:
                continue
            out.append(
                (
                    ((mx + dx) % 4) * 4 + (mz + dz) % 4,
                    ((mx - dx) % 4) * 4 + (mz - dz) % 4,
                )
            )
    return me, out


def greet(out):
    barrier = pltpu.get_barrier_semaphore()
    for to, _ in out:
        pl.semaphore_signal(
            barrier, inc=1, device_id={"dap": to}, device_id_type=pl.DeviceIdType.MESH
        )
    pl.semaphore_wait(barrier, len(out))


def exchange(src_ref, dst_ref, me, out, send_sem, recv_sem):
    copies = []
    for i, (to, _) in enumerate(out):
        copy = pltpu.make_async_remote_copy(
            src_ref=src_ref.at[to],
            dst_ref=dst_ref.at[me],
            send_sem=send_sem.at[i],
            recv_sem=recv_sem.at[i],
            device_id={"dap": to},
            device_id_type=pl.DeviceIdType.MESH,
        )
        copy.start()
        copies.append(copy)
    return copies


def spread(src, wide_ref, s):
    rows = pl.ds(pl.multiple_of(s * 16, 16), 16)
    for t in range(wide_ref.shape[0]):
        wide_ref[t, rows, :] = src[:, 128 * t : 128 * t + 128].astype(f32)


def low_lanes():
    return lax.broadcasted_iota(jnp.int32, (16, 128), 1) < 64


def gather_rows(wide_ref, first, m, stride, mat_ref, c, col):
    low = low_lanes()
    rows = pl.ds(first, 16, stride=stride)
    t0 = wide_ref[col, rows, :]
    t1 = wide_ref[col + 1, rows, :]
    t2 = wide_ref[col + 2, rows, :]
    r = 32 * m
    mat_ref[c, r : r + 16, 0:128] = t0.astype(bf16)
    mat_ref[c, r + 16 : r + 32, 0:128] = t1.astype(bf16)
    mat_ref[c, r : r + 16, 128:256] = jnp.where(low, t2, 0.0).astype(bf16)
    mat_ref[c, r + 16 : r + 32, 128:256] = jnp.where(low, pltpu.roll(t2, 64, 1), 0.0).astype(bf16)


def scatter_rows(res, m, wide_ref, first, stride, col):
    low = low_lanes()
    rows = pl.ds(first, 16, stride=stride)
    r = 32 * m
    wide_ref[col, rows, :] = res[r : r + 16, 0:128]
    wide_ref[col + 1, rows, :] = res[r + 16 : r + 32, 0:128]
    odd = pltpu.roll(res[r + 16 : r + 32, 128:256], 64, 1)
    wide_ref[col + 2, rows, :] = jnp.where(low, res[r : r + 16, 128:256], odd)


def clear_tail(ref):
    ref[:, RES:256, :] = jnp.zeros((CG, 256 - RES, 256), bf16)


def tri_kernel(transposed, ab_ref, x_ref, a_ref, b_ref, recv, wide, xwide, xs, s1, r1, s2, r2):
    me, out = peers()
    greet(out)
    copies = exchange(ab_ref, recv, me, out, s1, r1)
    clear_tail(a_ref)
    clear_tail(b_ref)
    spread(ab_ref[me], wide, me)
    for copy, (_, frm) in zip(copies, out):
        copy.wait_recv()
        spread(recv[frm], wide, frm)

    def channel(c, _):
        for m in range(STEPS):
            gather_rows(wide, c, m, 16, a_ref, c, 3 * m)
            gather_rows(wide, CG + c, m, 16, b_ref, c, 3 * m)
        k = 0 if transposed else 1
        res = dot(a_ref[c], b_ref[c], k, k)
        for m in range(STEPS):
            scatter_rows(res, m, xwide, c + CG * (m // 3), 16, 3 * (m % 3))
        return 0

    lax.fori_loop(0, CG, channel, 0)
    for copy in copies:
        copy.wait_send()
    for s in range(DEV):
        for t in range(9):
            xs[s, :, 128 * t : 128 * t + 128] = xwide[t, 16 * s : 16 * s + 16, :].astype(bf16)
    back = exchange(xs, x_ref, me, out, s2, r2)
    x_ref[me] = xs[me]
    for copy in back:
        copy.wait()


def grad_kernel(gx_ref, a_ref, b_ref, gab_ref, recv, wide, gmat, gwide, gs, s1, r1, s2, r2):
    me, out = peers()
    greet(out)
    copies = exchange(gx_ref, recv, me, out, s1, r1)
    clear_tail(gmat)
    spread(gx_ref[me], wide, me)
    for copy, (_, frm) in zip(copies, out):
        copy.wait_recv()
        spread(recv[frm], wide, frm)

    def channel(c, _):
        for m in range(STEPS):
            gather_rows(wide, c + CG * (m // 3), m, 16, gmat, c, 3 * (m % 3))
        ga = dot(b_ref[c], gmat[c], 1, 1)
        gb = dot(a_ref[c], gmat[c], 1, 0)
        for m in range(STEPS):
            scatter_rows(ga, m, gwide, c, 16, 3 * m)
            scatter_rows(gb, m, gwide, CG + c, 16, 3 * m)
        return 0

    lax.fori_loop(0, CG, channel, 0)
    for copy in copies:
        copy.wait_send()
    for s in range(DEV):
        for t in range(18):
            gs[s, :, 128 * t : 128 * t + 128] = gwide[t, 16 * s : 16 * s + 16, :].astype(bf16)
    back = exchange(gs, gab_ref, me, out, s2, r2)
    gab_ref[me] = gs[me]
    for copy in back:
        copy.wait()


def sum_kernel(part_ref, full_ref, vec_ref, recv, red, s1, r1, s2, r2):
    me, out = peers()
    greet(out)
    copies = exchange(part_ref, recv, me, out, s1, r1)
    recv[me] = part_ref[me]
    for copy in copies:
        copy.wait()
    total = recv[0].astype(f32)
    for s in range(1, DEV):
        total = total + recv[s].astype(f32)
    vec_ref[...] = total[48:64]
    red[...] = total[0:48].astype(bf16)
    back = []
    for i, (to, _) in enumerate(out):
        copy = pltpu.make_async_remote_copy(
            src_ref=red,
            dst_ref=full_ref.at[me],
            send_sem=s2.at[i],
            recv_sem=r2.at[i],
            device_id={"dap": to},
            device_id_type=pl.DeviceIdType.MESH,
        )
        copy.start()
        back.append(copy)
    full_ref[me] = red[...]
    for copy in back:
        copy.wait()


def shape(dims, dtype):
    return jax.ShapeDtypeStruct(dims, dtype)


def local_call(kernel, outs, *args):
    return pl.pallas_call(
        kernel,
        out_shape=outs,
        in_specs=[VM] * len(args),
        out_specs=[VM] * len(outs),
        compiler_params=pltpu.CompilerParams(vmem_limit_bytes=LIMIT),
    )(*args)


def link_call(kernel, outs, scratch, ident, *args):
    sems = [pltpu.SemaphoreType.DMA((DEV - 1,))] * 4
    return pl.pallas_call(
        kernel,
        out_shape=outs,
        in_specs=[VM] * len(args),
        out_specs=[VM] * len(outs),
        scratch_shapes=list(scratch) + sems,
        compiler_params=pltpu.CompilerParams(
            vmem_limit_bytes=LIMIT, collective_id=ident, has_side_effects=True
        ),
    )(*args)


def split_order(proj):
    return proj.reshape(CH, 2, 2, DEV, CG).transpose(2, 3, 1, 4, 0).reshape(4 * CH, CH)


def lane_order(rows, cols):
    order = cols.reshape(DEV, ROWS).T.reshape(RES)
    r = rows.reshape(STEPS, 2)
    row = jnp.concatenate(
        [jnp.broadcast_to(r[:, 0:1], (STEPS, 128)), jnp.broadcast_to(r[:, 1:2], (STEPS, 128)),
         jnp.broadcast_to(r[:, 0:1], (STEPS, 64)), jnp.broadcast_to(r[:, 1:2], (STEPS, 64))], axis=1)
    col = jnp.concatenate([order[:128], order[:128], order[128:], order[128:]])
    return row, jnp.broadcast_to(col[None], (STEPS, W))


def selector():
    lane = lax.broadcasted_iota(jnp.int32, (W, W), 1)
    src = lax.broadcasted_iota(jnp.int32, (W, W), 0)
    tail = lane - 256
    i = jnp.where(lane < 256, lane // 128, tail // 64)
    pos = jnp.where(lane < 256, lane % 128, 128 + tail % 64)
    res = (pos % DEV) * ROWS + pos // DEV
    return (src == i * RES + res).astype(bf16)


def shards(
    pair, cotangent, residue_mask, chain_ids, chain_embed, out_norm_gain, out_proj, out_gate,
    out_mid_gain, out_final, in_norm_gain, in_proj, in_gate, in_mid_gain, in_final,
):
    first = lax.axis_index("dap") * ROWS
    row_mask = lax.dynamic_slice_in_dim(residue_mask, first, ROWS, 0)
    row_chain = lax.dynamic_slice_in_dim(chain_ids, first, ROWS, 0)
    mr, mc = lane_order(row_mask, residue_mask)
    cr, cc = lane_order(row_chain, chain_ids)
    rows = jnp.stack([(mr * mc).astype(f32).reshape(PAIRS), (cr == cc).astype(f32).reshape(PAIRS)])
    zero = jnp.zeros_like(out_norm_gain)
    vec = jnp.stack(
        [chain_embed[0], chain_embed[1], out_norm_gain, out_mid_gain, in_norm_gain, in_mid_gain, zero, zero],
        axis=1,
    )
    sel = selector()
    w_out = jnp.concatenate([split_order(out_proj), out_gate.T], axis=0)
    w_in = split_order(in_proj)

    start, gate, ab = local_call(
        pre_kernel,
        [shape((CH, PAIRS), f32), shape((CH, PAIRS), f32), shape((DEV, 16, PAIRS), bf16)],
        pair, sel, rows, vec, w_out,
    )
    tri_scratch = [
        pltpu.VMEM((DEV, 16, PAIRS), bf16),
        pltpu.VMEM((18, DEV * 16, 128), f32),
        pltpu.VMEM((9, DEV * 16, 128), f32),
        pltpu.VMEM((DEV, 16, HALF), bf16),
    ]
    tri_out = [shape((DEV, 16, HALF), bf16), shape((CG, 256, 256), bf16), shape((CG, 256, 256), bf16)]
    x, _, _ = link_call(functools.partial(tri_kernel, False), tri_out, tri_scratch, 0, ab)
    mid, nrm, ab = local_call(
        mid_kernel,
        [shape((CH, PAIRS), bf16), shape((CH, PAIRS), bf16), shape((DEV, 16, PAIRS), bf16)],
        x, start, gate, rows, vec, out_final.T, w_in,
    )
    x, a, b = link_call(functools.partial(tri_kernel, True), tri_out, tri_scratch, 1, ab)
    gx, gl, ggate, gfinal, gmid = local_call(
        value_kernel,
        [shape((DEV, 16, HALF), bf16), shape((CH, PAIRS), bf16), shape((CH, CH), f32),
         shape((CH, CH), f32), shape((CH, 128), f32)],
        x, cotangent, nrm, sel, vec, in_gate.T, in_final.T, in_final,
    )
    (gab,) = link_call(
        grad_kernel,
        [shape((DEV, 16, PAIRS), bf16)],
        [
            pltpu.VMEM((DEV, 16, HALF), bf16),
            pltpu.VMEM((9, DEV * 16, 128), f32),
            pltpu.VMEM((CG, 256, 256), bf16),
            pltpu.VMEM((18, DEV * 16, 128), f32),
            pltpu.VMEM((DEV, 16, PAIRS), bf16),
        ],
        2, gx, a, b,
    )
    pair_grad, gproj, gnorm = local_call(
        post_kernel,
        [shape((ROWS, RES, CH), bf16), shape((4 * CH, CH), f32), shape((CH, 128), f32)],
        gab, cotangent, mid, nrm, gl, sel, rows, vec, w_in, w_in.T, in_gate,
    )

    flat = jnp.concatenate([gproj, ggate, gfinal], axis=0) * INV
    gains = jnp.stack([jnp.sum(gnorm, axis=1), jnp.sum(gmid, axis=1)]) * INV
    gains = jnp.concatenate([gains, jnp.zeros((14, CH), f32)], axis=0)
    part = jnp.concatenate(
        [flat.reshape(DEV, 48, CH), jnp.broadcast_to(gains[None], (DEV, 16, CH))], axis=1
    ).astype(bf16)
    full, gvec = link_call(
        sum_kernel,
        [shape((DEV, 48, CH), bf16), shape((16, CH), f32)],
        [pltpu.VMEM((DEV, 64, CH), bf16), pltpu.VMEM((48, CH), bf16)],
        3, part,
    )
    full = full.reshape(6 * CH, CH).astype(f32)
    grad_proj = (
        full[: 4 * CH].reshape(2, DEV, 2, CG, CH).transpose(4, 2, 0, 1, 3).reshape(CH, 4 * CH)
    )
    return (pair_grad, grad_proj, full[4 * CH : 5 * CH], full[5 * CH :], gvec[0], gvec[1])


def solution(mesh):
    whole = P()
    placed = (P("dap", "cplx", None), P("dap", "cplx", None), P("cplx"), P("cplx")) + (whole,) * 11
    return jax.shard_map(
        shards,
        mesh=mesh,
        in_specs=placed,
        out_specs=(
            P("dap", "cplx", None),
            P("cplx", None),
            P("cplx", None),
            P("cplx", None),
            P("cplx"),
            P("cplx"),
        ),
        check_vma=False,
    )
```

```python
import jax
import jax.numpy as jnp
from jax import lax
from jax.experimental import pallas as pl
from jax.experimental.pallas import tpu as pltpu
from jax.sharding import PartitionSpec as P

f32 = jnp.float32
bf16 = jnp.bfloat16

ROWS, RES, CH, DEV = 12, 192, 128, 16
CG = CH // DEV
W = 2 * RES
CHUNKS = 3
LANES = 2 * W
EPS = 1e-5
INV = 1.0 / RES
MESH = pl.DeviceIdType.MESH


def dot(a, b, ca, cb):
    return lax.dot_general(a, b, (((ca,), (cb,)), ((), ())), preferred_element_type=f32)


def norm_stats(v):
    mean = jnp.mean(v, axis=0, keepdims=True)
    cent = v - mean
    var = jnp.mean(cent * cent, axis=0, keepdims=True)
    rstd = lax.rsqrt(var + EPS)
    return cent * rstd, rstd


def norm_grad(gh, xhat, rstd):
    return rstd * (
        gh
        - jnp.mean(gh, axis=0, keepdims=True)
        - xhat * jnp.mean(gh * xhat, axis=0, keepdims=True)
    )


def sig(v):
    return jax.nn.sigmoid(v)


def lane_sum(v):
    total = v[:, 0:128]
    for t in range(1, v.shape[1] // 128):
        total = total + v[:, 128 * t : 128 * t + 128]
    return total


def low(rows):
    return lax.broadcasted_iota(jnp.int32, (rows, 128), 1) < 64


def swap(v):
    return pltpu.roll(v, 64, 1)


def selector():
    lane = lax.broadcasted_iota(jnp.int32, (W, W), 1)
    src = lax.broadcasted_iota(jnp.int32, (W, W), 0)
    tail = lane - 256
    first = lane < 256
    i = jnp.where(first, lane >> 7, tail >> 6)
    pos = jnp.where(first, lane & 127, 128 + (tail & 63))
    res = (pos & (DEV - 1)) * ROWS + (pos >> 4)
    return jnp.where(src == i * RES + res, 1.0, 0.0).astype(bf16)


def turn(w):
    return w.astype(f32).T.astype(bf16)


def kernel(
    pair, cot, mask_row, chain_row, mask_s, chain_s, embed, gain0, gain1, gain2, gain3,
    w_out, w_og, w_of, w_in, w_ig, w_if,
    out, o_proj, o_gate, o_final, o_norm, o_mid,
    sel, vecs, cols, wt_out, wt_og, wt_of, wt_in, wt_ig, wt_if,
    start, gate, mid, nrm, gl, cott,
    b1s, a1s, x1s, b2s, a2s, x2s, gxs, gas, gbs, p1s, p2s, g1s, g2s,
    b1r, a1r, x1r, b2r, a2r, x2r, gxr, gar, gbr, p1r, p2r, g1r, g2r,
    wide, back, am, bm, aq, b2, gq, acc_proj, acc_gate, acc_final, acc_norm, acc_mid,
    send_sem, recv_sem,
):
    me = lax.axis_index("dap")
    mx, mz = me // 4, me % 4

    def peer(i):
        o = 15 - i
        return ((mx + o % 4) % 4) * 4 + (mz + o // 4) % 4

    barrier = pltpu.get_barrier_semaphore()

    def greet(i, _):
        pl.semaphore_signal(barrier, inc=1, device_id={"dap": peer(i)}, device_id_type=MESH)
        return 0

    lax.fori_loop(0, DEV - 1, greet, 0)

    def send(src, dst, r, ident):
        def one(i, _):
            to = peer(i)
            pltpu.make_async_remote_copy(
                src_ref=src.at[r, to],
                dst_ref=dst.at[r, me],
                send_sem=send_sem.at[ident, r],
                recv_sem=recv_sem.at[ident, r],
                device_id={"dap": to},
                device_id_type=MESH,
            ).start()
            return 0

        lax.fori_loop(0, DEV - 1, one, 0)
        dst[r, me] = src[r, me]

    def share(src, dst, ident):
        def one(i, _):
            pltpu.make_async_remote_copy(
                src_ref=src,
                dst_ref=dst.at[me],
                send_sem=send_sem.at[ident, 0],
                recv_sem=recv_sem.at[ident, 0],
                device_id={"dap": peer(i)},
                device_id_type=MESH,
            ).start()
            return 0

        lax.fori_loop(0, DEV - 1, one, 0)
        dst[me] = src[...]

    def wait(dst, r, ident):
        blocks = dst.at[r, pl.ds(0, DEV - 1)]
        pltpu.make_async_copy(blocks, blocks, recv_sem.at[ident, r]).wait()

    sel[...] = selector()
    vecs[...] = jnp.zeros_like(vecs)
    vecs[0:2, :] = embed[...]
    vecs[2:3, :] = gain0[...]
    vecs[3:4, :] = gain1[...]
    vecs[4:5, :] = gain2[...]
    vecs[5:6, :] = gain3[...]
    cols[...] = vecs[...].T
    for t in range(4):
        wt_out[128 * t : 128 * t + 128, :] = turn(w_out[:, 128 * t : 128 * t + 128])
    wt_og[...] = turn(w_og[...])

    def by_lane(row_ref):
        wide_row = jnp.broadcast_to(row_ref[...].astype(f32), (16, RES)).astype(bf16)
        return (dot(wide_row, sel[0:RES, :], 1, 0) + dot(wide_row, sel[RES:W, :], 1, 0))[0:1]

    lane = lax.broadcasted_iota(jnp.int32, (1, W), 1)
    second = jnp.where(lane < 256, lane >> 7, (lane - 256) >> 6) == 1
    lane_mask = by_lane(mask_row)
    lane_chain = by_lane(chain_row)

    def row_pair(ref, m):
        at = me * ROWS + 2 * m
        return jnp.where(second, ref[0, at + 1].astype(f32), ref[0, at].astype(f32))

    def pair_mask(m):
        return row_pair(mask_s, m) * lane_mask

    def to_channels(ref, m):
        return dot(ref[pl.ds(2 * m, 2)].reshape(W, CH), sel[...], 0, 0)

    def blocks(v):
        return v.reshape(DEV, CG, v.shape[1]).astype(bf16)

    pl.semaphore_wait(barrier, DEV - 1)

    def project(r, _):
        for mm in (0, 1):
            m = 2 * r + mm
            at = slice(W * mm, W * mm + W)
            same = row_pair(chain_s, m) == lane_chain
            st = to_channels(pair, m) + jnp.where(same, cols[:, 1:2], cols[:, 0:1])
            start[m] = st
            xhat, _ = norm_stats(st)
            normed = (xhat * cols[:, 2:3]).astype(bf16)
            p = dot(wt_out[...], normed, 1, 0)
            pm = pair_mask(m)
            b1s[r, :, :, at] = blocks(pm * sig(p[256:384]) * p[384:512])
            a1s[r, :, :, at] = blocks(pm * sig(p[0:128]) * p[128:256])
            gate[m] = sig(dot(wt_og[...], normed, 1, 0))
        send(b1s, b1r, r, 0)
        return 0

    lax.fori_loop(0, CHUNKS, project, 0)

    def send_all(src, dst, ident):
        def one(r, _):
            send(src, dst, r, ident)
            return 0

        lax.fori_loop(0, CHUNKS, one, 0)

    send_all(a1s, a1r, 1)

    for t in range(4):
        wt_in[128 * t : 128 * t + 128, :] = turn(w_in[:, 128 * t : 128 * t + 128])
    wt_of[...] = turn(w_of[...])
    wt_ig[...] = turn(w_ig[...])
    wt_if[...] = turn(w_if[...])

    def turn_cot(m, _):
        cott[m] = to_channels(cot, m).astype(bf16)
        return 0

    lax.fori_loop(0, 2 * CHUNKS, turn_cot, 0)
    bm[:, RES:256, :] = jnp.zeros((CG, 256 - RES, 256), bf16)
    gq[...] = jnp.zeros_like(gq)

    def widen(src, r):
        for t in range(LANES // 128):
            wide[t] = src[r, :, :, 128 * t : 128 * t + 128].astype(f32).reshape(CH, 128)

    def fill_rows(c, put):
        pick = pl.ds(c, DEV, stride=CG)
        lo = low(DEV)
        for mm in (0, 1):
            tail = wide[3 * mm + 2, pick, :]
            put(32 * mm, wide[3 * mm, pick, :], jnp.where(lo, tail, 0.0))
            put(32 * mm + 16, wide[3 * mm + 1, pick, :], jnp.where(lo, swap(tail), 0.0))

    def rows_into(mat, r, c):
        base = r * 64

        def put(row, head, tail):
            at = pl.ds(pl.multiple_of(base + row, 16), 16)
            mat[c, at, 0:128] = head.astype(bf16)
            mat[c, at, 128:256] = tail.astype(bf16)

        fill_rows(c, put)

    def take_rows(src, r, mat):
        widen(src, r)

        def one(c, _):
            rows_into(mat, r, c)
            return 0

        lax.fori_loop(0, CG, one, 0)

    def rows_out(res, c):
        pick = pl.ds(c, DEV, stride=CG)
        lo = low(DEV)
        for mm in (0, 1):
            r = 32 * mm
            back[3 * mm, pick, :] = res[r : r + 16, 0:128]
            back[3 * mm + 1, pick, :] = res[r + 16 : r + 32, 0:128]
            back[3 * mm + 2, pick, :] = jnp.where(
                lo, res[r : r + 16, 128:256], swap(res[r + 16 : r + 32, 128:256])
            )

    def flush(dst, r):
        for t in range(LANES // 128):
            dst[r, :, :, 128 * t : 128 * t + 128] = back[t].reshape(DEV, CG, 128).astype(bf16)

    def take_b1(r, _):
        wait(b1r, r, 0)
        take_rows(b1r, r, bm)
        return 0

    lax.fori_loop(0, CHUNKS, take_b1, 0)

    def product_out(r, _):
        wait(a1r, r, 1)
        widen(a1r, r)

        def one(c, _):
            rows_into(am, r, c)
            rows = pl.ds(pl.multiple_of(r * 64, 64), 64)
            rows_out(dot(am[c, rows, :], bm[c], 1, 1), c)
            return 0

        lax.fori_loop(0, CG, one, 0)
        flush(x1s, r)
        send(x1s, x1r, r, 2)
        return 0

    lax.fori_loop(0, CHUNKS, product_out, 0)

    def columns_of(t0, t1):
        lo = low(CH)
        return jnp.where(lo, t0, swap(t1)), jnp.where(lo, swap(t0), t1)

    def middle(r, _):
        wait(x1r, r, 2)
        for mm in (0, 1):
            m = 2 * r + mm
            at = slice(W * mm, W * mm + W)
            xhat, _ = norm_stats(x1r[r, :, :, at].astype(f32).reshape(CH, W))
            y = (xhat * cols[:, 3:4]).astype(bf16)
            md = (start[m] + gate[m] * dot(wt_of[...], y, 1, 0)).astype(bf16)
            mid[m] = md
            zhat, _ = norm_stats(md.astype(f32))
            normed = (zhat * cols[:, 4:5]).astype(bf16)
            nrm[m] = normed
            p = dot(wt_in[...], normed, 1, 0)
            pm = pair_mask(m)
            b2s[r, :, :, at] = blocks(pm * sig(p[256:384]) * p[384:512])
            a = pm * sig(p[0:128]) * p[128:256]
            q0, q1 = columns_of(a[:, 0:128], a[:, 128:256])
            tile = pl.ds(pl.multiple_of(m * 128, 128), 128)
            a2s[0, :, :, tile] = blocks(q0)
            a2s[1, :, :, tile] = blocks(q1)
            a2s[2, :, :, tile] = blocks(a[:, 256:384])
        send(b2s, b2r, r, 3)
        return 0

    lax.fori_loop(0, CHUNKS, middle, 0)
    send_all(a2s, a2r, 4)

    def take_b2(r, _):
        wait(b2r, r, 3)
        take_rows(b2r, r, b2)
        return 0

    lax.fori_loop(0, CHUNKS, take_b2, 0)

    def product_in(q, _):
        wait(a2r, q, 4)
        widen(a2r, q)

        def one(c, _):
            pick = pl.ds(c, DEV, stride=CG)
            lo = low(DEV)
            for m in range(2 * CHUNKS):
                t = wide[m, pick, :]
                aq[q, c, 32 * m : 32 * m + 16, :] = jnp.where(lo, t, 0.0).astype(bf16)
                aq[q, c, 32 * m + 16 : 32 * m + 32, :] = jnp.where(lo, swap(t), 0.0).astype(bf16)
            rows_out(dot(aq[q, c], b2[c], 0, 0), c)
            return 0

        lax.fori_loop(0, CG, one, 0)
        flush(x2s, q)
        send(x2s, x2r, q, 5)
        return 0

    lax.fori_loop(0, CHUNKS, product_in, 0)

    acc_gate[...] = jnp.zeros_like(acc_gate)
    acc_final[...] = jnp.zeros_like(acc_final)
    acc_mid[...] = jnp.zeros_like(acc_mid)
    acc_proj[...] = jnp.zeros_like(acc_proj)
    acc_norm[...] = jnp.zeros_like(acc_norm)

    def values(r, _):
        wait(x2r, r, 5)
        for mm in (0, 1):
            m = 2 * r + mm
            at = slice(W * mm, W * mm + W)
            xhat, rstd = norm_stats(x2r[r, :, :, at].astype(f32).reshape(CH, W))
            gain = cols[:, 5:6]
            y = (xhat * gain).astype(bf16)
            normed = nrm[m]
            ct = cott[m].astype(f32)
            s = sig(dot(wt_ig[...], normed, 1, 0))
            value = dot(wt_if[...], y, 1, 0)
            gv = (ct * s).astype(bf16)
            gy = dot(w_if[...], gv, 1, 0)
            gx = norm_grad(gy * gain, xhat, rstd)
            gxs[r, :, :, at] = blocks(gx)
            glm = (ct * value * s * (1.0 - s)).astype(bf16)
            gl[m] = glm
            acc_final[...] += dot(y, gv, 1, 1)
            acc_gate[...] += dot(normed, glm, 1, 1)
            acc_mid[...] += lane_sum(gy * xhat)
        send(gxs, gxr, r, 6)
        return 0

    lax.fori_loop(0, CHUNKS, values, 0)
    p1s[0, :, :, 0:128] = blocks(acc_gate[...] * INV)
    p1s[0, :, :, 128:256] = blocks(acc_final[...] * INV)
    send(p1s, p1r, 0, 9)

    def grad_a(q, _):
        wait(gxr, q, 6)
        widen(gxr, q)

        def one(c, _):
            def put(row, head, tail):
                gq[q, c, row : row + 16, 0:128] = head.astype(bf16)
                gq[q, c, row : row + 16, 128:256] = tail.astype(bf16)

            fill_rows(c, put)
            res = dot(b2[c], gq[q, c], 1, 1)
            pick = pl.ds(c, DEV, stride=CG)
            lo = low(DEV)
            for m in range(2 * CHUNKS):
                back[m, pick, :] = jnp.where(
                    lo, res[32 * m : 32 * m + 16], swap(res[32 * m + 16 : 32 * m + 32])
                )
            return 0

        lax.fori_loop(0, CG, one, 0)
        flush(gas, q)
        send(gas, gar, q, 7)
        return 0

    lax.fori_loop(0, CHUNKS, grad_a, 0)

    def grad_b(r, _):
        rows = pl.ds(pl.multiple_of(r * 64, 64), 64)

        def one(c, _):
            res = dot(aq[0, c, rows, :], gq[0, c], 1, 0)
            for q in (1, 2):
                res = res + dot(aq[q, c, rows, :], gq[q, c], 1, 0)
            rows_out(res, c)
            return 0

        lax.fori_loop(0, CG, one, 0)
        flush(gbs, r)
        send(gbs, gbr, r, 8)
        return 0

    lax.fori_loop(0, CHUNKS, grad_b, 0)

    wait(p1r, 0, 9)
    total = p1r[0, 0].astype(f32)
    for s in range(1, DEV):
        total = total + p1r[0, s].astype(f32)
    g1s[...] = total.astype(bf16)
    share(g1s, g1r, 11)

    def wait_ga(q, _):
        wait(gar, q, 7)
        return 0

    lax.fori_loop(0, CHUNKS, wait_ga, 0)

    def finish(r, _):
        wait(gbr, r, 8)
        for mm in (0, 1):
            m = 2 * r + mm
            at = slice(W * mm, W * mm + W)
            normed = nrm[m]
            p = dot(wt_in[...], normed, 1, 0)
            pm = pair_mask(m)
            gb = gbr[r, :, :, at].astype(f32).reshape(CH, W) * pm
            tile = pl.ds(pl.multiple_of(m * 128, 128), 128)
            q0 = gar[0, :, :, tile].astype(f32).reshape(CH, 128)
            q1 = gar[1, :, :, tile].astype(f32).reshape(CH, 128)
            q2 = gar[2, :, :, tile].astype(f32).reshape(CH, 128)
            t0, t1 = columns_of(q0, q1)
            ga = jnp.concatenate([t0, t1, q2], axis=1) * pm
            sa = sig(p[0:128])
            sb = sig(p[256:384])
            gp = jnp.concatenate(
                [
                    ga * p[128:256] * sa * (1.0 - sa),
                    ga * sa,
                    gb * p[384:512] * sb * (1.0 - sb),
                    gb * sb,
                ],
                axis=0,
            ).astype(bf16)
            acc_proj[...] += dot(normed, gp, 1, 1)
            gn = dot(w_in[...], gp, 1, 0) + dot(w_ig[...], gl[m], 1, 0)
            zhat, rstd = norm_stats(mid[m].astype(f32))
            acc_norm[...] += lane_sum(gn * zhat)
            gz = norm_grad(gn * cols[:, 4:5], zhat, rstd)
            res = (cott[m].astype(f32) + gz).astype(bf16)
            out[pl.ds(2 * m, 2)] = dot(sel[...], res, 1, 1).astype(bf16).reshape(2, RES, CH)
        return 0

    lax.fori_loop(0, CHUNKS, finish, 0)

    p2s[0, :, :, 0:512] = blocks(acc_proj[...] * INV)
    gains = jnp.concatenate(
        [
            jnp.sum(acc_norm[...].T, axis=0, keepdims=True),
            jnp.sum(acc_mid[...].T, axis=0, keepdims=True),
            jnp.zeros((CG - 2, 128), f32),
        ],
        axis=0,
    )
    p2s[0, :, :, 512:640] = jnp.broadcast_to((gains * INV)[None], (DEV, CG, 128)).astype(bf16)
    send(p2s, p2r, 0, 10)
    wait(p2r, 0, 10)
    total = p2r[0, 0].astype(f32)
    for s in range(1, DEV):
        total = total + p2r[0, s].astype(f32)
    o_norm[...] = total[0:1, 512:640]
    o_mid[...] = total[1:2, 512:640]
    g2s[...] = total[:, 0:512].astype(bf16)
    share(g2s, g2r, 12)

    for ident, ref in ((11, g1r), (12, g2r)):
        got = ref.at[pl.ds(0, DEV - 1)]
        pltpu.make_async_copy(got, got, recv_sem.at[ident, 0]).wait()
    o_proj[...] = g2r[...].astype(f32).reshape(CH, 512)
    both = g1r[...].astype(f32).reshape(CH, 256)
    o_gate[...] = both[:, 0:128]
    o_final[...] = both[:, 128:256]

    for ident, ref in (
        (0, b1s), (1, a1s), (2, x1s), (3, b2s), (4, a2s), (5, x2s), (6, gxs), (7, gas), (8, gbs),
    ):
        for r in range(CHUNKS):
            sent = ref.at[r, pl.ds(0, DEV - 1)]
            pltpu.make_async_copy(sent, sent, send_sem.at[ident, r]).wait()
    for ident, ref in ((9, p1s), (10, p2s)):
        sent = ref.at[0, pl.ds(0, DEV - 1)]
        pltpu.make_async_copy(sent, sent, send_sem.at[ident, 0]).wait()
    for ident, ref in ((11, g1r), (12, g2r)):
        sent = ref.at[pl.ds(0, DEV - 1)]
        pltpu.make_async_copy(sent, sent, send_sem.at[ident, 0]).wait()


def shards(
    pair, cotangent, residue_mask, chain_ids, chain_embed, out_norm_gain, out_proj, out_gate,
    out_mid_gain, out_final, in_norm_gain, in_proj, in_gate, in_mid_gain, in_final,
):
    vm = pl.BlockSpec(memory_space=pltpu.VMEM)
    sm = pl.BlockSpec(memory_space=pltpu.SMEM)
    v = pltpu.VMEM
    wire = v((CHUNKS, DEV, CG, LANES), bf16)
    steps = lambda dtype: v((2 * CHUNKS, CH, W), dtype)
    part1, part2 = v((1, DEV, CG, 256), bf16), v((1, DEV, CG, 640), bf16)
    square = v((CH, CH), bf16)
    scratch = (
        [v((W, W), bf16), v((CH, 128), f32), v((CH, 128), f32)]
        + [v((4 * CH, CH), bf16), square, square, v((4 * CH, CH), bf16), square, square]
        + [steps(f32), steps(f32), steps(bf16), steps(bf16), steps(bf16), steps(bf16)]
        + [wire] * 9 + [part1, part2, v((CG, 256), bf16), v((CG, 512), bf16)]
        + [wire] * 9 + [part1, part2, v((DEV, CG, 256), bf16), v((DEV, CG, 512), bf16)]
        + [v((LANES // 128, CH, 128), f32)] * 2
        + [v((CG, RES, 256), bf16), v((CG, 256, 256), bf16)]
        + [v((CHUNKS, CG, RES, 128), bf16), v((CG, RES, 256), bf16), v((CHUNKS, CG, 128, 256), bf16)]
        + [v((CH, 512), f32)] + [v((CH, CH), f32)] * 4
        + [pltpu.SemaphoreType.DMA((13, CHUNKS))] * 2
    )
    mask = residue_mask.reshape(1, RES)
    chain = chain_ids.reshape(1, RES)
    gains = [g.reshape(1, CH) for g in (out_norm_gain, out_mid_gain, in_norm_gain, in_mid_gain)]
    outs = [
        jax.ShapeDtypeStruct((ROWS, RES, CH), bf16),
        jax.ShapeDtypeStruct((CH, 512), f32),
        jax.ShapeDtypeStruct((CH, CH), f32),
        jax.ShapeDtypeStruct((CH, CH), f32),
        jax.ShapeDtypeStruct((1, CH), f32),
        jax.ShapeDtypeStruct((1, CH), f32),
    ]
    got = pl.pallas_call(
        kernel,
        out_shape=outs,
        in_specs=[vm] * 4 + [sm] * 2 + [vm] * 11,
        out_specs=[vm] * 6,
        scratch_shapes=scratch,
        compiler_params=pltpu.CompilerParams(
            vmem_limit_bytes=60 * 1024 * 1024, collective_id=0, has_side_effects=True
        ),
    )(
        pair, cotangent, mask, chain, mask, chain, chain_embed, *gains,
        out_proj, out_gate, out_final, in_proj, in_gate, in_final,
    )
    return (*got[:4], got[4].reshape(CH), got[5].reshape(CH))


def solution(mesh):
    whole = P()
    placed = (P("dap", "cplx", None), P("dap", "cplx", None), P("cplx"), P("cplx")) + (whole,) * 11
    return jax.shard_map(
        shards,
        mesh=mesh,
        in_specs=placed,
        out_specs=(
            P("dap", "cplx", None),
            P("cplx", None),
            P("cplx", None),
            P("cplx", None),
            P("cplx"),
            P("cplx"),
        ),
        check_vma=False,
    )
```

```python
import jax
import jax.numpy as jnp
from jax import lax
from jax.experimental import pallas as pl
from jax.experimental.pallas import tpu as pltpu
from jax.sharding import PartitionSpec as P

f32 = jnp.float32
bf16 = jnp.bfloat16

ROWS, RES, CH, DEV = 12, 192, 128, 16
CG = CH // DEV
HDEV = DEV // 2
HG = CH // HDEV
W = 2 * RES
CHUNKS = 3
LANES = 2 * W
EPS = 1e-5
INV = 1.0 / RES
MESH = pl.DeviceIdType.MESH


def dot(a, b, ca, cb):
    return lax.dot_general(a, b, (((ca,), (cb,)), ((), ())), preferred_element_type=f32)


def norm_stats(v):
    mean = jnp.mean(v, axis=0, keepdims=True)
    cent = v - mean
    var = jnp.mean(cent * cent, axis=0, keepdims=True)
    rstd = lax.rsqrt(var + EPS)
    return cent * rstd, rstd


def norm_grad(gh, xhat, rstd):
    return rstd * (
        gh
        - jnp.mean(gh, axis=0, keepdims=True)
        - xhat * jnp.mean(gh * xhat, axis=0, keepdims=True)
    )


def sig(v):
    return jax.nn.sigmoid(v)


def lane_sum(v):
    total = v[:, 0:128]
    for t in range(1, v.shape[1] // 128):
        total = total + v[:, 128 * t : 128 * t + 128]
    return total


def low(rows):
    return lax.broadcasted_iota(jnp.int32, (rows, 128), 1) < 64


def swap(v):
    return pltpu.roll(v, 64, 1)


def selector():
    lane = lax.broadcasted_iota(jnp.int32, (W, W), 1)
    src = lax.broadcasted_iota(jnp.int32, (W, W), 0)
    tail = lane - 256
    first = lane < 256
    i = jnp.where(first, lane >> 7, tail >> 6)
    pos = jnp.where(first, lane & 127, 128 + (tail & 63))
    res = (pos & (DEV - 1)) * ROWS + (pos >> 4)
    return jnp.where(src == i * RES + res, 1.0, 0.0).astype(bf16)


def turn(w):
    return w.astype(f32).T.astype(bf16)


def kernel(
    pair_h, cot_h, mask_h, chain_h, embed_h, gain0_h, gain1_h, gain2_h, gain3_h,
    w_out_h, w_og_h, w_of_h, w_in_h, w_ig_h, w_if_h,
    out, o_all,
    pair, cot, mask_row, chain_row, embed, gain0, gain1, gain2, gain3,
    w_out, w_og, w_of, w_in, w_ig, w_if, mask_s, chain_s, outv, gps,
    sel, vecs, cols, wt_out, wt_og, wt_of, wt_in, wt_ig, wt_if,
    start, gate, mid, nrm, gl, cott,
    b1s, a1s, x1s, b2s, a2s, x2s, gxs, gas, gbs, p1s, p2s, g1s, g2s,
    b1r, a1r, x1r, b2r, a2r, x2r, gxr, gar, gbr, p1r, p2r, g1r, g2r,
    wide, back, bm, aq, b2, gq, acc_proj, acc_gate, acc_final, acc_norm, acc_mid,
    send_sem, recv_sem, load_sem, out_sem,
):
    me = lax.axis_index("dap")
    mx, mz = me // 4, me % 4

    def peer(i):
        o = 15 - i
        return ((mx + o % 4) % 4) * 4 + (mz + o // 4) % 4

    mine = mx * 2 + mz % 2

    def seat(to):
        return (to // 4) * 2 + to % 2

    def near(i):
        o = HDEV - 1 - i
        return ((mx + o % 4) % 4) * 4 + (mz // 2) * 2 + (mz + o // 4) % 2

    barrier = pltpu.get_barrier_semaphore()

    def greet(i, _):
        pl.semaphore_signal(barrier, inc=1, device_id={"dap": peer(i)}, device_id_type=MESH)
        return 0

    lax.fori_loop(0, DEV - 1, greet, 0)

    loads = [
        pltpu.make_async_copy(src, dst, load_sem.at[i])
        for i, (src, dst) in enumerate(
            (
                (embed_h, embed), (gain0_h, gain0), (gain1_h, gain1), (gain2_h, gain2),
                (gain3_h, gain3), (w_og_h, w_og), (w_out_h, w_out),
                (mask_h, mask_row), (chain_h, chain_row), (mask_h, mask_s), (chain_h, chain_s),
                (pair_h, pair), (cot_h, cot),
                (w_of_h, w_of), (w_in_h, w_in), (w_ig_h, w_ig), (w_if_h, w_if),
            )
        )
    ]
    for load in loads:
        load.start()

    def send(src, dst, r, ident):
        def one(i, _):
            to = peer(i)
            pltpu.make_async_remote_copy(
                src_ref=src.at[r, to],
                dst_ref=dst.at[r, me],
                send_sem=send_sem.at[ident, r],
                recv_sem=recv_sem.at[ident, r],
                device_id={"dap": to},
                device_id_type=MESH,
            ).start()
            return 0

        lax.fori_loop(0, DEV - 1, one, 0)
        dst[r, me] = src[r, me]

    def send_half(src, dst, r, ident, count, partner, slot):
        def one(i, _):
            to = partner(i)
            pltpu.make_async_remote_copy(
                src_ref=src.at[r, seat(to)],
                dst_ref=dst.at[r, slot],
                send_sem=send_sem.at[ident, r],
                recv_sem=recv_sem.at[ident, r],
                device_id={"dap": to},
                device_id_type=MESH,
            ).start()
            return 0

        lax.fori_loop(0, count, one, 0)
        dst[r, slot] = src[r, mine]

    def share(src, dst, ident):
        def one(i, _):
            pltpu.make_async_remote_copy(
                src_ref=src,
                dst_ref=dst.at[me],
                send_sem=send_sem.at[ident, 0],
                recv_sem=recv_sem.at[ident, 0],
                device_id={"dap": peer(i)},
                device_id_type=MESH,
            ).start()
            return 0

        lax.fori_loop(0, DEV - 1, one, 0)
        dst[me] = src[...]

    def wait(dst, r, ident):
        blocks = dst.at[r, pl.ds(0, dst.shape[1] - 1)]
        pltpu.make_async_copy(blocks, blocks, recv_sem.at[ident, r]).wait()

    sel[...] = selector()
    vecs[...] = jnp.zeros_like(vecs)
    for load in loads[:11]:
        load.wait()
    vecs[0:2, :] = embed[...]
    vecs[2:3, :] = gain0[...]
    vecs[3:4, :] = gain1[...]
    vecs[4:5, :] = gain2[...]
    vecs[5:6, :] = gain3[...]
    cols[...] = vecs[...].T
    for t in range(4):
        wt_out[128 * t : 128 * t + 128, :] = turn(w_out[:, 128 * t : 128 * t + 128])
    wt_og[...] = turn(w_og[...])

    def by_lane(row_ref):
        wide_row = jnp.broadcast_to(row_ref[...].astype(f32), (16, RES)).astype(bf16)
        return (dot(wide_row, sel[0:RES, :], 1, 0) + dot(wide_row, sel[RES:W, :], 1, 0))[0:1]

    lane = lax.broadcasted_iota(jnp.int32, (1, W), 1)
    second = jnp.where(lane < 256, lane >> 7, (lane - 256) >> 6) == 1
    lane_mask = by_lane(mask_row)
    lane_chain = by_lane(chain_row)

    def row_pair(ref, m):
        at = me * ROWS + 2 * m
        return jnp.where(second, ref[0, at + 1].astype(f32), ref[0, at].astype(f32))

    def pair_mask(m):
        return row_pair(mask_s, m) * lane_mask

    def to_channels(ref, m):
        return dot(ref[pl.ds(2 * m, 2)].reshape(W, CH), sel[...], 0, 0)

    def blocks(v):
        return v.reshape(DEV, CG, v.shape[1]).astype(bf16)

    def half_blocks(v):
        return v.reshape(HDEV, HG, v.shape[1]).astype(bf16)

    loads[11].wait()

    def project(r, _):
        for mm in (0, 1):
            m = 2 * r + mm
            at = slice(W * mm, W * mm + W)
            same = row_pair(chain_s, m) == lane_chain
            st = to_channels(pair, m) + jnp.where(same, cols[:, 1:2], cols[:, 0:1])
            start[m] = st
            xhat, _ = norm_stats(st)
            normed = (xhat * cols[:, 2:3]).astype(bf16)
            p = dot(wt_out[...], normed, 1, 0)
            pm = pair_mask(m)
            b1s[r, :, :, at] = half_blocks(pm * sig(p[256:384]) * p[384:512])
            a1s[r, :, :, at] = half_blocks(pm * sig(p[0:128]) * p[128:256])
            gate[m] = sig(dot(wt_og[...], normed, 1, 0))
        return 0

    lax.fori_loop(0, CHUNKS, project, 0)
    pl.semaphore_wait(barrier, DEV - 1)

    def send_b1(r, _):
        send_half(b1s, b1r, r, 0, DEV - 1, peer, me)
        return 0

    def send_a1(r, _):
        send_half(a1s, a1r, r, 1, HDEV - 1, near, mine)
        return 0

    def sent(ref, r, ident):
        blocks_out = ref.at[r, pl.ds(0, ref.shape[1] - 1)]
        pltpu.make_async_copy(blocks_out, blocks_out, send_sem.at[ident, r]).wait()

    lax.fori_loop(0, CHUNKS, send_b1, 0)
    send_a1(0, 0)

    for load in loads[12:]:
        load.wait()
    for t in range(4):
        wt_in[128 * t : 128 * t + 128, :] = turn(w_in[:, 128 * t : 128 * t + 128])
    wt_of[...] = turn(w_of[...])
    wt_ig[...] = turn(w_ig[...])
    wt_if[...] = turn(w_if[...])

    def turn_cot(m, _):
        cott[m] = to_channels(cot, m).astype(bf16)
        return 0

    lax.fori_loop(0, 2 * CHUNKS, turn_cot, 0)
    bm[:, RES:256, :] = jnp.zeros((HG, 256 - RES, 256), bf16)

    def channels(count, body, width=4):
        def group(g, _):
            for u in range(width):
                body(g * width + u)
            return 0

        lax.fori_loop(0, count // width, group, 0)

    def widen(src, r):
        rows = src.shape[1] * src.shape[2]
        for t in range(LANES // 128):
            tile = src[r, :, :, 128 * t : 128 * t + 128].astype(f32)
            wide[t, 0:rows, :] = tile.reshape(rows, 128)

    def fill_rows(c, put, stride=CG):
        pick = pl.ds(c, DEV, stride=stride)
        lo = low(DEV)
        for mm in (0, 1):
            tail = wide[3 * mm + 2, pick, :]
            put(32 * mm, wide[3 * mm, pick, :], jnp.where(lo, tail, 0.0))
            put(32 * mm + 16, wide[3 * mm + 1, pick, :], jnp.where(lo, swap(tail), 0.0))

    def rows_into(mat, r, c, stride):
        base = r * 64

        def put(row, head, tail):
            at = pl.ds(pl.multiple_of(base + row, 16), 16)
            mat[c, at, 0:128] = head.astype(bf16)
            mat[c, at, 128:256] = tail.astype(bf16)

        fill_rows(c, put, stride)

    def take_rows(src, r, mat):
        widen(src, r)
        count = src.shape[2]

        channels(count, lambda c: rows_into(mat, r, c, count))

    def rows_out(res, c):
        pick = pl.ds(c, DEV, stride=CG)
        lo = low(DEV)
        for mm in (0, 1):
            r = 32 * mm
            back[3 * mm, pick, :] = res[r : r + 16, 0:128]
            back[3 * mm + 1, pick, :] = res[r + 16 : r + 32, 0:128]
            back[3 * mm + 2, pick, :] = jnp.where(
                lo, res[r : r + 16, 128:256], swap(res[r + 16 : r + 32, 128:256])
            )

    def flush(dst, r):
        for t in range(LANES // 128):
            tile = back[t].reshape(dst.shape[1], dst.shape[2], 128)
            dst[r, :, :, 128 * t : 128 * t + 128] = tile.astype(bf16)

    def take_b1(r):
        wait(b1r, r, 0)
        take_rows(b1r, r, bm)

    take_b1(0)
    lax.fori_loop(1, CHUNKS, send_a1, 0)
    take_b1(1)
    take_b1(2)

    def product_out(r, _):
        wait(a1r, r, 1)
        widen(a1r, r)

        def one(c):
            pick = pl.ds(c, HDEV, stride=HG)
            lo = low(HDEV)
            parts = []
            for mm in (0, 1):
                tail = wide[3 * mm + 2, pick, :]
                heads = jnp.concatenate([wide[3 * mm, pick, :], wide[3 * mm + 1, pick, :]], axis=0)
                tails = jnp.concatenate(
                    [jnp.where(lo, tail, 0.0), jnp.where(lo, swap(tail), 0.0)], axis=0
                )
                parts.append(jnp.concatenate([heads, tails], axis=1))
            rows = jnp.concatenate(parts, axis=0).astype(bf16)
            res = dot(rows, bm[c], 1, 1)
            for mm in (0, 1):
                u = 16 * mm
                back[3 * mm, pick, :] = res[u : u + 8, 0:128]
                back[3 * mm + 1, pick, :] = res[u + 8 : u + 16, 0:128]
                back[3 * mm + 2, pick, :] = jnp.where(
                    lo, res[u : u + 8, 128:256], swap(res[u + 8 : u + 16, 128:256])
                )

        channels(HG, one)
        flush(x1s, r)
        send_half(x1s, x1r, r, 2, HDEV - 1, near, mine)
        return 0

    lax.fori_loop(0, CHUNKS, product_out, 0)

    def columns_of(t0, t1):
        lo = low(CH)
        return jnp.where(lo, t0, swap(t1)), jnp.where(lo, swap(t0), t1)

    def middle(r, _):
        wait(x1r, r, 2)
        for mm in (0, 1):
            m = 2 * r + mm
            at = slice(W * mm, W * mm + W)
            xhat, _ = norm_stats(x1r[r, :, :, at].astype(f32).reshape(CH, W))
            y = (xhat * cols[:, 3:4]).astype(bf16)
            md = (start[m] + gate[m] * dot(wt_of[...], y, 1, 0)).astype(bf16)
            mid[m] = md
            zhat, _ = norm_stats(md.astype(f32))
            normed = (zhat * cols[:, 4:5]).astype(bf16)
            nrm[m] = normed
            p = dot(wt_in[...], normed, 1, 0)
            pm = pair_mask(m)
            b2s[r, :, :, at] = blocks(pm * sig(p[256:384]) * p[384:512])
            a = pm * sig(p[0:128]) * p[128:256]
            q0, q1 = columns_of(a[:, 0:128], a[:, 128:256])
            tile = pl.ds(pl.multiple_of(m * 128, 128), 128)
            a2s[0, :, :, tile] = blocks(q0)
            a2s[1, :, :, tile] = blocks(q1)
            a2s[2, :, :, tile] = blocks(a[:, 256:384])
        send(b2s, b2r, r, 3)
        return 0

    lax.fori_loop(0, CHUNKS, middle, 0)
    send(a2s, a2r, 0, 4)

    for r in range(CHUNKS):
        if r > 0:
            sent(b2s, r, 3)
            send(a2s, a2r, r, 4)
        wait(b2r, r, 3)
        take_rows(b2r, r, b2)

    def product_in(q, _):
        wait(a2r, q, 4)
        widen(a2r, q)

        def one(c):
            pick = pl.ds(c, DEV, stride=CG)
            lo = low(DEV)
            parts = []
            for m in range(2 * CHUNKS):
                t = wide[m, pick, :]
                parts.append(jnp.where(lo, t, 0.0).astype(bf16))
                parts.append(jnp.where(lo, swap(t), 0.0).astype(bf16))
            cols_q = jnp.concatenate(parts, axis=0)
            aq[q, c] = cols_q
            rows_out(dot(cols_q, b2[c], 0, 0), c)

        channels(CG, one)
        flush(x2s, q)
        send(x2s, x2r, q, 5)
        return 0

    lax.fori_loop(0, CHUNKS, product_in, 0)

    acc_gate[...] = jnp.zeros_like(acc_gate)
    acc_final[...] = jnp.zeros_like(acc_final)
    acc_mid[...] = jnp.zeros_like(acc_mid)
    acc_proj[...] = jnp.zeros_like(acc_proj)
    acc_norm[...] = jnp.zeros_like(acc_norm)

    def values(r, _):
        wait(x2r, r, 5)
        for mm in (0, 1):
            m = 2 * r + mm
            at = slice(W * mm, W * mm + W)
            xhat, rstd = norm_stats(x2r[r, :, :, at].astype(f32).reshape(CH, W))
            gain = cols[:, 5:6]
            y = (xhat * gain).astype(bf16)
            normed = nrm[m]
            ct = cott[m].astype(f32)
            s = sig(dot(wt_ig[...], normed, 1, 0))
            value = dot(wt_if[...], y, 1, 0)
            gv = (ct * s).astype(bf16)
            gy = dot(w_if[...], gv, 1, 0)
            gx = norm_grad(gy * gain, xhat, rstd)
            gxs[r, :, :, at] = blocks(gx)
            glm = (ct * value * s * (1.0 - s)).astype(bf16)
            gl[m] = glm
            acc_final[...] += dot(y, gv, 1, 1)
            acc_gate[...] += dot(normed, glm, 1, 1)
            acc_mid[...] += lane_sum(gy * xhat)
        send(gxs, gxr, r, 6)
        return 0

    lax.fori_loop(0, CHUNKS, values, 0)
    p1s[0, :, :, 0:128] = blocks(acc_gate[...] * INV)
    p1s[0, :, :, 128:256] = blocks(acc_final[...] * INV)
    send(p1s, p1r, 0, 9)

    def grad_a(q, _):
        wait(gxr, q, 6)
        widen(gxr, q)

        def one(c):
            parts = []

            def put(row, head, tail):
                parts.append(jnp.concatenate([head, tail], axis=1).astype(bf16))

            fill_rows(c, put)
            parts.append(jnp.zeros((64, 256), bf16))
            rows_q = jnp.concatenate(parts, axis=0)
            gq[q, c] = rows_q
            res = dot(b2[c], rows_q, 1, 1)
            pick = pl.ds(c, DEV, stride=CG)
            lo = low(DEV)
            for m in range(2 * CHUNKS):
                back[m, pick, :] = jnp.where(
                    lo, res[32 * m : 32 * m + 16], swap(res[32 * m + 16 : 32 * m + 32])
                )

        channels(CG, one)
        flush(gas, q)
        send(gas, gar, q, 7)
        return 0

    lax.fori_loop(0, CHUNKS, grad_a, 0)

    def grad_b(r):
        rows = pl.ds(pl.multiple_of(r * 64, 64), 64)

        def one(c):
            res = dot(aq[0, c, rows, :], gq[0, c], 1, 0)
            for q in (1, 2):
                res = res + dot(aq[q, c, rows, :], gq[q, c], 1, 0)
            rows_out(res, c)

        channels(CG, one)
        flush(gbs, r)
        send(gbs, gbr, r, 8)

    for r in range(CHUNKS):
        grad_b(r)

    wait(p1r, 0, 9)
    total = p1r[0, 0].astype(f32)
    for s in range(1, DEV):
        total = total + p1r[0, s].astype(f32)
    g1s[...] = total.astype(bf16)
    share(g1s, g1r, 11)

    def wait_ga(q, _):
        wait(gar, q, 7)
        return 0

    lax.fori_loop(0, CHUNKS, wait_ga, 0)

    def finish(r, _):
        wait(gbr, r, 8)
        for mm in (0, 1):
            m = 2 * r + mm
            at = slice(W * mm, W * mm + W)
            normed = nrm[m]
            p = dot(wt_in[...], normed, 1, 0)
            pm = pair_mask(m)
            gb = gbr[r, :, :, at].astype(f32).reshape(CH, W) * pm
            tile = pl.ds(pl.multiple_of(m * 128, 128), 128)
            q0 = gar[0, :, :, tile].astype(f32).reshape(CH, 128)
            q1 = gar[1, :, :, tile].astype(f32).reshape(CH, 128)
            q2 = gar[2, :, :, tile].astype(f32).reshape(CH, 128)
            t0, t1 = columns_of(q0, q1)
            ga = jnp.concatenate([t0, t1, q2], axis=1) * pm
            sa = sig(p[0:128])
            sb = sig(p[256:384])
            gp = jnp.concatenate(
                [
                    ga * p[128:256] * sa * (1.0 - sa),
                    ga * sa,
                    gb * p[384:512] * sb * (1.0 - sb),
                    gb * sb,
                ],
                axis=0,
            ).astype(bf16)
            gps[m] = gp
            acc_proj[...] += dot(normed, gp, 1, 1)
        return 0

    lax.fori_loop(0, CHUNKS, finish, 0)
    p2s[0] = blocks(acc_proj[...] * INV)
    send(p2s, p2r, 0, 10)

    def deliver_pair(m):
        rows = pl.ds(2 * m, 2)
        return pltpu.make_async_copy(outv.at[rows], out.at[rows], out_sem.at[m])

    def last(m, _):
        gn = dot(w_in[...], gps[m], 1, 0) + dot(w_ig[...], gl[m], 1, 0)
        zhat, rstd = norm_stats(mid[m].astype(f32))
        acc_norm[...] += lane_sum(gn * zhat)
        gz = norm_grad(gn * cols[:, 4:5], zhat, rstd)
        res = (cott[m].astype(f32) + gz).astype(bf16)
        outv[pl.ds(2 * m, 2)] = dot(sel[...], res, 1, 1).astype(bf16).reshape(2, RES, CH)
        deliver_pair(m).start()
        return 0

    lax.fori_loop(0, 2 * CHUNKS, last, 0)

    gains = jnp.concatenate(
        [
            jnp.sum(acc_norm[...].T, axis=0, keepdims=True),
            jnp.sum(acc_mid[...].T, axis=0, keepdims=True),
            jnp.zeros((CG - 2, 128), f32),
        ],
        axis=0,
    )
    g2s[:, 512:640] = (gains * INV).astype(bf16)
    wait(p2r, 0, 10)
    total = p2r[0, 0].astype(f32)
    for s in range(1, DEV):
        total = total + p2r[0, s].astype(f32)
    g2s[:, 0:512] = total.astype(bf16)
    share(g2s, g2r, 12)
    for m in range(2 * CHUNKS):
        deliver_pair(m).wait()

    for ident, ref in ((11, g1r), (12, g2r)):
        got = ref.at[pl.ds(0, DEV - 1)]
        pltpu.make_async_copy(got, got, recv_sem.at[ident, 0]).wait()
    o_all[0:CH, 0:512] = g2r[:, :, 0:512].astype(f32).reshape(CH, 512)
    total = g2r[0, :, 512:640].astype(f32)
    for s in range(1, DEV):
        total = total + g2r[s, :, 512:640].astype(f32)
    o_all[CH : CH + CG, 0:128] = total
    o_all[0:CH, 512:768] = g1r[...].astype(f32).reshape(CH, 256)

    for ident, ref, rest in (
        (0, b1r, (0, 1, 2)), (1, a1s, (0, 1, 2)), (2, x1s, (0, 1, 2)), (3, b2s, (0,)),
        (4, a2s, (0, 1, 2)), (5, x2s, (0, 1, 2)), (6, gxs, (0, 1, 2)), (7, gas, (0, 1, 2)),
        (8, gbs, (0, 1, 2)),
        (9, p1s, (0,)), (10, p2s, (0,)),
    ):
        for r in rest:
            sent(ref, r, ident)
    for ident, ref in ((11, g1r), (12, g2r)):
        gone = ref.at[pl.ds(0, DEV - 1)]
        pltpu.make_async_copy(gone, gone, send_sem.at[ident, 0]).wait()


def deliver(pair_in, all_in, pair_out, proj, gate, final, norm, mid):
    pair_out[...] = pair_in[...]
    proj[...] = all_in[0:CH, 0:512]
    gate[...] = all_in[0:CH, 512:640]
    final[...] = all_in[0:CH, 640:768]
    norm[...] = all_in[CH : CH + 1, 0:128]
    mid[...] = all_in[CH + 1 : CH + 2, 0:128]


def shards(
    pair, cotangent, residue_mask, chain_ids, chain_embed, out_norm_gain, out_proj, out_gate,
    out_mid_gain, out_final, in_norm_gain, in_proj, in_gate, in_mid_gain, in_final,
):
    vm = pl.BlockSpec(memory_space=pltpu.VMEM)
    hbm = pl.BlockSpec(memory_space=pl.ANY)
    v = pltpu.VMEM
    wire = v((CHUNKS, DEV, CG, LANES), bf16)
    half = v((CHUNKS, HDEV, HG, LANES), bf16)
    twice = v((CHUNKS, DEV, HG, LANES), bf16)
    steps = lambda dtype: v((2 * CHUNKS, CH, W), dtype)
    part1, part2 = v((1, DEV, CG, 256), bf16), v((1, DEV, CG, 512), bf16)
    square = v((CH, CH), bf16)
    block = v((ROWS, RES, CH), bf16)
    scratch = (
        [block, block] + [v((1, RES), jnp.int32)] * 2 + [v((2, CH), f32)] + [v((1, CH), f32)] * 4
        + [v((CH, 512), bf16), square, square, v((CH, 512), bf16), square, square]
        + [pltpu.SMEM((1, RES), jnp.int32)] * 2 + [block, v((2 * CHUNKS, 4 * CH, W), bf16)]
        + [v((W, W), bf16), v((CH, 128), f32), v((CH, 128), f32)]
        + [v((4 * CH, CH), bf16), square, square, v((4 * CH, CH), bf16), square, square]
        + [steps(f32), steps(f32), steps(bf16), steps(bf16), steps(bf16), steps(bf16)]
        + [half] * 3 + [wire] * 6 + [part1, part2, v((CG, 256), bf16), v((CG, 640), bf16)]
        + [twice, half, half] + [wire] * 6 + [part1, part2, v((DEV, CG, 256), bf16), v((DEV, CG, 640), bf16)]
        + [v((LANES // 128, DEV * HG, 128), f32), v((LANES // 128, CH, 128), f32)]
        + [v((HG, 256, 256), bf16)]
        + [v((CHUNKS, CG, RES, 128), bf16), v((CG, RES, 256), bf16), v((CHUNKS, CG, 128, 256), bf16)]
        + [v((CH, 512), f32)] + [v((CH, CH), f32)] * 4
        + [pltpu.SemaphoreType.DMA((13, CHUNKS))] * 2
        + [pltpu.SemaphoreType.DMA((17,)), pltpu.SemaphoreType.DMA((2 * CHUNKS,))]
    )
    mask = residue_mask.reshape(1, RES)
    chain = chain_ids.reshape(1, RES)
    gains = [g.reshape(1, CH) for g in (out_norm_gain, out_mid_gain, in_norm_gain, in_mid_gain)]
    outs = [
        jax.ShapeDtypeStruct((ROWS, RES, CH), bf16),
        jax.ShapeDtypeStruct((CH, 512), f32),
        jax.ShapeDtypeStruct((CH, CH), f32),
        jax.ShapeDtypeStruct((CH, CH), f32),
        jax.ShapeDtypeStruct((1, CH), f32),
        jax.ShapeDtypeStruct((1, CH), f32),
    ]
    params = pltpu.CompilerParams(
        vmem_limit_bytes=60 * 1024 * 1024, collective_id=0, has_side_effects=True
    )
    got = pl.pallas_call(
        kernel,
        out_shape=[outs[0], jax.ShapeDtypeStruct((CH + CG, 768), f32)],
        in_specs=[hbm] * 15,
        out_specs=[hbm, vm],
        scratch_shapes=scratch,
        compiler_params=params,
    )(
        pair, cotangent, mask, chain, chain_embed, *gains,
        out_proj, out_gate, out_final, in_proj, in_gate, in_final,
    )
    got = pl.pallas_call(deliver, out_shape=outs, in_specs=[vm] * 2, out_specs=[vm] * 6)(*got)
    return (*got[:4], got[4].reshape(CH), got[5].reshape(CH))


def solution(mesh):
    whole = P()
    placed = (P("dap", "cplx", None), P("dap", "cplx", None), P("cplx"), P("cplx")) + (whole,) * 11
    return jax.shard_map(
        shards,
        mesh=mesh,
        in_specs=placed,
        out_specs=(
            P("dap", "cplx", None),
            P("cplx", None),
            P("cplx", None),
            P("cplx", None),
            P("cplx"),
            P("cplx"),
        ),
        check_vma=False,
    )
```

```python
import jax
import jax.numpy as jnp
from jax import lax
from jax.experimental import pallas as pl
from jax.experimental.pallas import tpu as pltpu
from jax.sharding import PartitionSpec as P

f32 = jnp.float32
bf16 = jnp.bfloat16

ROWS, RES, CH, DEV = 12, 192, 128, 16
CG = CH // DEV
HDEV = DEV // 2
HG = CH // HDEV
W = 2 * RES
CHUNKS = 3
LANES = 2 * W
EPS = 1e-5
INV = 1.0 / RES
MESH = pl.DeviceIdType.MESH


def dot(a, b, ca, cb):
    return lax.dot_general(a, b, (((ca,), (cb,)), ((), ())), preferred_element_type=f32)


def norm_stats(v):
    mean = jnp.mean(v, axis=0, keepdims=True)
    cent = v - mean
    var = jnp.mean(cent * cent, axis=0, keepdims=True)
    rstd = lax.rsqrt(var + EPS)
    return cent * rstd, rstd


def norm_grad(gh, xhat, rstd):
    return rstd * (
        gh
        - jnp.mean(gh, axis=0, keepdims=True)
        - xhat * jnp.mean(gh * xhat, axis=0, keepdims=True)
    )


def sig(v):
    return jax.nn.sigmoid(v)


def lane_sum(v):
    total = v[:, 0:128]
    for t in range(1, v.shape[1] // 128):
        total = total + v[:, 128 * t : 128 * t + 128]
    return total


def low(rows):
    return lax.broadcasted_iota(jnp.int32, (rows, 128), 1) < 64


def swap(v):
    return pltpu.roll(v, 64, 1)


def selector():
    lane = lax.broadcasted_iota(jnp.int32, (W, W), 1)
    src = lax.broadcasted_iota(jnp.int32, (W, W), 0)
    tail = lane - 256
    first = lane < 256
    i = jnp.where(first, lane >> 7, tail >> 6)
    pos = jnp.where(first, lane & 127, 128 + (tail & 63))
    res = (pos & (DEV - 1)) * ROWS + (pos >> 4)
    return jnp.where(src == i * RES + res, 1.0, 0.0).astype(bf16)


def turn(w):
    return w.astype(f32).T.astype(bf16)


def kernel(
    pair_h, cot_h, mask_h, chain_h, embed_h, gain0_h, gain1_h, gain2_h, gain3_h,
    w_out_h, w_og_h, w_of_h, w_in_h, w_ig_h, w_if_h,
    out, o_all,
    pair, cot, mask_row, chain_row, embed, gain0, gain1, gain2, gain3,
    w_out, w_og, w_of, w_in, w_ig, w_if, mask_s, chain_s, outv, gps,
    sel, vecs, cols, wt_out, wt_og, wt_of, wt_in, wt_ig, wt_if,
    start, gate, mid, nrm, gl, cott,
    b1s, a1s, x1s, b2s, a2s, x2s, gxs, gas, gbs, p1s, p2s, p3s, g1s, g2s, g3s, h1s, h3s,
    b1r, a1r, x1r, b2r, a2r, x2r, gxr, gar, gbr, p1r, p2r, p3r, g1r, g2r, g3r, h1r, h3r,
    wide, back, bm, aq, b2, gq, acc_left, acc_right, acc_gate, acc_final, acc_norm, acc_mid,
    send_sem, recv_sem, load_sem, out_sem,
):
    me = lax.axis_index("dap")
    mx, mz = me // 4, me % 4

    def peer(i):
        k = i // 4
        d = 2 + k - (k // 2) * (2 * k - 1)
        z = (mz // 2 + d // 2) % 2 * 2 + (mz + d) % 2
        return ((mx + 3 - i % 4) % 4) * 4 + z

    mine = mx * 2 + mz % 2

    def seat(to):
        return (to // 4) * 2 + to % 2

    def near(i):
        o = HDEV - 1 - i
        return ((mx + o % 4) % 4) * 4 + (mz // 2) * 2 + (mz + o // 4) % 2

    barrier = pltpu.get_barrier_semaphore()

    def greet(i, _):
        pl.semaphore_signal(barrier, inc=1, device_id={"dap": peer(i)}, device_id_type=MESH)
        return 0

    lax.fori_loop(0, DEV - 1, greet, 0)

    loads = [
        pltpu.make_async_copy(src, dst, load_sem.at[i])
        for i, (src, dst) in enumerate(
            (
                (embed_h, embed), (gain0_h, gain0), (gain1_h, gain1), (gain2_h, gain2),
                (gain3_h, gain3), (w_og_h, w_og), (w_out_h, w_out),
                (mask_h, mask_row), (chain_h, chain_row), (mask_h, mask_s), (chain_h, chain_s),
                (pair_h, pair), (cot_h, cot),
                (w_of_h, w_of), (w_in_h, w_in), (w_ig_h, w_ig), (w_if_h, w_if),
            )
        )
    ]
    for load in loads:
        load.start()

    def send(src, dst, r, ident):
        def one(i, _):
            to = peer(i)
            pltpu.make_async_remote_copy(
                src_ref=src.at[r, to],
                dst_ref=dst.at[r, me],
                send_sem=send_sem.at[ident, r],
                recv_sem=recv_sem.at[ident, r],
                device_id={"dap": to},
                device_id_type=MESH,
            ).start()
            return 0

        lax.fori_loop(0, DEV - 1, one, 0)
        dst[r, me] = src[r, me]

    def send_half(src, dst, r, ident, count, partner, slot):
        def one(i, _):
            to = partner(i)
            pltpu.make_async_remote_copy(
                src_ref=src.at[r, seat(to)],
                dst_ref=dst.at[r, slot],
                send_sem=send_sem.at[ident, r],
                recv_sem=recv_sem.at[ident, r],
                device_id={"dap": to},
                device_id_type=MESH,
            ).start()
            return 0

        lax.fori_loop(0, count, one, 0)
        dst[r, slot] = src[r, mine]

    def share(src, dst, ident):
        def one(i, _):
            pltpu.make_async_remote_copy(
                src_ref=src,
                dst_ref=dst.at[me],
                send_sem=send_sem.at[ident, 0],
                recv_sem=recv_sem.at[ident, 0],
                device_id={"dap": peer(i)},
                device_id_type=MESH,
            ).start()
            return 0

        lax.fori_loop(0, DEV - 1, one, 0)
        dst[me] = src[...]

    def share_half(src, dst, ident):
        def one(i, _):
            pltpu.make_async_remote_copy(
                src_ref=src,
                dst_ref=dst.at[mine],
                send_sem=send_sem.at[ident, 0],
                recv_sem=recv_sem.at[ident, 0],
                device_id={"dap": near(i)},
                device_id_type=MESH,
            ).start()
            return 0

        lax.fori_loop(0, HDEV - 1, one, 0)
        dst[mine] = src[...]

    def across(src, dst, ident):
        return pltpu.make_async_remote_copy(
            src_ref=src,
            dst_ref=dst,
            send_sem=send_sem.at[ident, 0],
            recv_sem=recv_sem.at[ident, 0],
            device_id={"dap": mx * 4 + (mz + 2) % 4},
            device_id_type=MESH,
        )

    def summed(ref, count):
        total = ref[0].astype(f32)
        for k in range(1, count):
            total = total + ref[k].astype(f32)
        return total

    def wait(dst, r, ident):
        blocks = dst.at[r, pl.ds(0, dst.shape[1] - 1)]
        pltpu.make_async_copy(blocks, blocks, recv_sem.at[ident, r]).wait()

    sel[...] = selector()
    vecs[...] = jnp.zeros_like(vecs)
    for load in loads[:11]:
        load.wait()
    vecs[0:2, :] = embed[...]
    vecs[2:3, :] = gain0[...]
    vecs[3:4, :] = gain1[...]
    vecs[4:5, :] = gain2[...]
    vecs[5:6, :] = gain3[...]
    cols[...] = vecs[...].T
    for t in range(4):
        wt_out[128 * t : 128 * t + 128, :] = turn(w_out[:, 128 * t : 128 * t + 128])
    wt_og[...] = turn(w_og[...])

    def by_lane(row_ref):
        wide_row = jnp.broadcast_to(row_ref[...].astype(f32), (16, RES)).astype(bf16)
        return (dot(wide_row, sel[0:RES, :], 1, 0) + dot(wide_row, sel[RES:W, :], 1, 0))[0:1]

    lane = lax.broadcasted_iota(jnp.int32, (1, W), 1)
    second = jnp.where(lane < 256, lane >> 7, (lane - 256) >> 6) == 1
    lane_mask = by_lane(mask_row)
    lane_chain = by_lane(chain_row)

    def row_pair(ref, m):
        at = me * ROWS + 2 * m
        return jnp.where(second, ref[0, at + 1].astype(f32), ref[0, at].astype(f32))

    def pair_mask(m):
        return row_pair(mask_s, m) * lane_mask

    def to_channels(ref, m):
        return dot(ref[pl.ds(2 * m, 2)].reshape(W, CH), sel[...], 0, 0)

    def blocks(v):
        return v.reshape(DEV, CG, v.shape[1]).astype(bf16)

    def half_blocks(v):
        return v.reshape(HDEV, HG, v.shape[1]).astype(bf16)

    loads[11].wait()

    def project(r, _):
        for mm in (0, 1):
            m = 2 * r + mm
            at = slice(W * mm, W * mm + W)
            same = row_pair(chain_s, m) == lane_chain
            st = to_channels(pair, m) + jnp.where(same, cols[:, 1:2], cols[:, 0:1])
            start[m] = st
            xhat, _ = norm_stats(st)
            normed = (xhat * cols[:, 2:3]).astype(bf16)
            p = dot(wt_out[...], normed, 1, 0)
            pm = pair_mask(m)
            b1s[r, :, :, at] = half_blocks(pm * sig(p[256:384]) * p[384:512])
            a1s[r, :, :, at] = half_blocks(pm * sig(p[0:128]) * p[128:256])
            gate[m] = sig(dot(wt_og[...], normed, 1, 0))
        return 0

    project(0, 0)
    pl.semaphore_wait(barrier, DEV - 1)

    def send_b1(r, _):
        send_half(b1s, b1r, r, 0, DEV - 1, peer, me)
        return 0

    def send_a1(r, _):
        send_half(a1s, a1r, r, 1, HDEV - 1, near, mine)
        return 0

    def sent(ref, r, ident):
        blocks_out = ref.at[r, pl.ds(0, ref.shape[1] - 1)]
        pltpu.make_async_copy(blocks_out, blocks_out, send_sem.at[ident, r]).wait()

    send_b1(0, 0)

    def project_and_send(r, _):
        project(r, 0)
        send_b1(r, 0)
        return 0

    lax.fori_loop(1, CHUNKS, project_and_send, 0)
    send_a1(0, 0)

    for load in loads[12:]:
        load.wait()
    for t in range(4):
        wt_in[128 * t : 128 * t + 128, :] = turn(w_in[:, 128 * t : 128 * t + 128])
    wt_of[...] = turn(w_of[...])
    wt_ig[...] = turn(w_ig[...])
    wt_if[...] = turn(w_if[...])

    def turn_cot(m, _):
        cott[m] = to_channels(cot, m).astype(bf16)
        return 0

    lax.fori_loop(0, 2 * CHUNKS, turn_cot, 0)
    bm[:, RES:256, :] = jnp.zeros((HG, 256 - RES, 256), bf16)

    def channels(count, body, width=4):
        def group(g, _):
            for u in range(width):
                body(g * width + u)
            return 0

        lax.fori_loop(0, count // width, group, 0)

    def widen(src, r):
        rows = src.shape[1] * src.shape[2]
        for t in range(LANES // 128):
            tile = src[r, :, :, 128 * t : 128 * t + 128].astype(f32)
            wide[t, 0:rows, :] = tile.reshape(rows, 128)

    def fill_rows(c, put, stride=CG):
        pick = pl.ds(c, DEV, stride=stride)
        lo = low(DEV)
        for mm in (0, 1):
            tail = wide[3 * mm + 2, pick, :]
            put(32 * mm, wide[3 * mm, pick, :], jnp.where(lo, tail, 0.0))
            put(32 * mm + 16, wide[3 * mm + 1, pick, :], jnp.where(lo, swap(tail), 0.0))

    def rows_into(mat, r, c, stride):
        base = r * 64

        def put(row, head, tail):
            at = pl.ds(pl.multiple_of(base + row, 16), 16)
            mat[c, at, 0:128] = head.astype(bf16)
            mat[c, at, 128:256] = tail.astype(bf16)

        fill_rows(c, put, stride)

    def take_rows(src, r, mat):
        widen(src, r)
        count = src.shape[2]

        channels(count, lambda c: rows_into(mat, r, c, count))

    def rows_out(res, c):
        pick = pl.ds(c, DEV, stride=CG)
        lo = low(DEV)
        for mm in (0, 1):
            r = 32 * mm
            back[3 * mm, pick, :] = res[r : r + 16, 0:128]
            back[3 * mm + 1, pick, :] = res[r + 16 : r + 32, 0:128]
            back[3 * mm + 2, pick, :] = jnp.where(
                lo, res[r : r + 16, 128:256], swap(res[r + 16 : r + 32, 128:256])
            )

    def flush(dst, r):
        for t in range(LANES // 128):
            tile = back[t].reshape(dst.shape[1], dst.shape[2], 128)
            dst[r, :, :, 128 * t : 128 * t + 128] = tile.astype(bf16)

    def take_b1(r):
        wait(b1r, r, 0)
        take_rows(b1r, r, bm)

    take_b1(0)
    lax.fori_loop(1, CHUNKS, send_a1, 0)
    take_b1(1)
    take_b1(2)

    def product_out(r, _):
        wait(a1r, r, 1)
        widen(a1r, r)

        def one(c):
            pick = pl.ds(c, HDEV, stride=HG)
            lo = low(HDEV)
            parts = []
            for mm in (0, 1):
                tail = wide[3 * mm + 2, pick, :]
                heads = jnp.concatenate([wide[3 * mm, pick, :], wide[3 * mm + 1, pick, :]], axis=0)
                tails = jnp.concatenate(
                    [jnp.where(lo, tail, 0.0), jnp.where(lo, swap(tail), 0.0)], axis=0
                )
                parts.append(jnp.concatenate([heads, tails], axis=1))
            rows = jnp.concatenate(parts, axis=0).astype(bf16)
            res = dot(rows, bm[c], 1, 1)
            for mm in (0, 1):
                u = 16 * mm
                back[3 * mm, pick, :] = res[u : u + 8, 0:128]
                back[3 * mm + 1, pick, :] = res[u + 8 : u + 16, 0:128]
                back[3 * mm + 2, pick, :] = jnp.where(
                    lo, res[u : u + 8, 128:256], swap(res[u + 8 : u + 16, 128:256])
                )

        channels(HG, one)
        flush(x1s, r)
        send_half(x1s, x1r, r, 2, HDEV - 1, near, mine)
        return 0

    lax.fori_loop(0, CHUNKS, product_out, 0)

    def columns_of(t0, t1):
        lo = low(CH)
        return jnp.where(lo, t0, swap(t1)), jnp.where(lo, swap(t0), t1)

    def middle(r, _):
        wait(x1r, r, 2)
        for mm in (0, 1):
            m = 2 * r + mm
            at = slice(W * mm, W * mm + W)
            xhat, _ = norm_stats(x1r[r, :, :, at].astype(f32).reshape(CH, W))
            y = (xhat * cols[:, 3:4]).astype(bf16)
            md = (start[m] + gate[m] * dot(wt_of[...], y, 1, 0)).astype(bf16)
            mid[m] = md
            zhat, _ = norm_stats(md.astype(f32))
            normed = (zhat * cols[:, 4:5]).astype(bf16)
            nrm[m] = normed
            p = dot(wt_in[...], normed, 1, 0)
            pm = pair_mask(m)
            b2s[r, :, :, at] = blocks(pm * sig(p[256:384]) * p[384:512])
            a = pm * sig(p[0:128]) * p[128:256]
            q0, q1 = columns_of(a[:, 0:128], a[:, 128:256])
            tile = pl.ds(pl.multiple_of(m * 128, 128), 128)
            a2s[0, :, :, tile] = blocks(q0)
            a2s[1, :, :, tile] = blocks(q1)
            a2s[2, :, :, tile] = blocks(a[:, 256:384])
        send(b2s, b2r, r, 3)
        return 0

    lax.fori_loop(0, CHUNKS, middle, 0)
    send(a2s, a2r, 0, 4)

    for r in range(CHUNKS):
        if r > 0:
            sent(b2s, r, 3)
            send(a2s, a2r, r, 4)
        wait(b2r, r, 3)
        take_rows(b2r, r, b2)

    def product_in(q, _):
        wait(a2r, q, 4)
        widen(a2r, q)

        def one(c):
            pick = pl.ds(c, DEV, stride=CG)
            lo = low(DEV)
            parts = []
            for m in range(2 * CHUNKS):
                t = wide[m, pick, :]
                parts.append(jnp.where(lo, t, 0.0).astype(bf16))
                parts.append(jnp.where(lo, swap(t), 0.0).astype(bf16))
            cols_q = jnp.concatenate(parts, axis=0)
            aq[q, c] = cols_q
            rows_out(dot(cols_q, b2[c], 0, 0), c)

        channels(CG, one)
        flush(x2s, q)
        send(x2s, x2r, q, 5)
        return 0

    lax.fori_loop(0, CHUNKS, product_in, 0)

    acc_gate[...] = jnp.zeros_like(acc_gate)
    acc_final[...] = jnp.zeros_like(acc_final)
    acc_mid[...] = jnp.zeros_like(acc_mid)
    acc_left[...] = jnp.zeros_like(acc_left)
    acc_right[...] = jnp.zeros_like(acc_right)
    acc_norm[...] = jnp.zeros_like(acc_norm)

    def values(r, _):
        wait(x2r, r, 5)
        for mm in (0, 1):
            m = 2 * r + mm
            at = slice(W * mm, W * mm + W)
            xhat, rstd = norm_stats(x2r[r, :, :, at].astype(f32).reshape(CH, W))
            gain = cols[:, 5:6]
            y = (xhat * gain).astype(bf16)
            normed = nrm[m]
            ct = cott[m].astype(f32)
            s = sig(dot(wt_ig[...], normed, 1, 0))
            value = dot(wt_if[...], y, 1, 0)
            gv = (ct * s).astype(bf16)
            gy = dot(w_if[...], gv, 1, 0)
            gx = norm_grad(gy * gain, xhat, rstd)
            gxs[r, :, :, at] = blocks(gx)
            glm = (ct * value * s * (1.0 - s)).astype(bf16)
            gl[m] = glm
            acc_final[...] += dot(y, gv, 1, 1)
            acc_gate[...] += dot(normed, glm, 1, 1)
            acc_mid[...] += lane_sum(gy * xhat)
        send(gxs, gxr, r, 6)
        return 0

    lax.fori_loop(0, CHUNKS, values, 0)
    p1s[0, :, :, 0:128] = half_blocks(acc_gate[...] * INV)
    p1s[0, :, :, 128:256] = half_blocks(acc_final[...] * INV)
    send_half(p1s, p1r, 0, 9, HDEV - 1, near, mine)

    def sum_half(src, half_sum, other, ident, next_ident):
        wait(src, 0, ident)
        half_sum[...] = summed(src.at[0], HDEV).astype(bf16)
        across(half_sum, other, next_ident).start()

    def sum_both(half_sum, other, full, result, ident, next_ident):
        across(half_sum, other, ident).wait_recv()
        full[...] = (half_sum[...].astype(f32) + other[...].astype(f32)).astype(bf16)
        share_half(full, result, next_ident)

    def grad_a(q, _):
        wait(gxr, q, 6)
        widen(gxr, q)

        def one(c):
            parts = []

            def put(row, head, tail):
                parts.append(jnp.concatenate([head, tail], axis=1).astype(bf16))

            fill_rows(c, put)
            parts.append(jnp.zeros((64, 256), bf16))
            rows_q = jnp.concatenate(parts, axis=0)
            gq[q, c] = rows_q
            res = dot(b2[c], rows_q, 1, 1)
            pick = pl.ds(c, DEV, stride=CG)
            lo = low(DEV)
            for m in range(2 * CHUNKS):
                back[m, pick, :] = jnp.where(
                    lo, res[32 * m : 32 * m + 16], swap(res[32 * m + 16 : 32 * m + 32])
                )

        channels(CG, one)
        flush(gas, q)
        send(gas, gar, q, 7)
        return 0

    lax.fori_loop(0, CHUNKS, grad_a, 0)

    def grad_b(r):
        rows = pl.ds(pl.multiple_of(r * 64, 64), 64)

        def one(c):
            res = dot(aq[0, c, rows, :], gq[0, c], 1, 0)
            for q in (1, 2):
                res = res + dot(aq[q, c, rows, :], gq[q, c], 1, 0)
            rows_out(res, c)

        channels(CG, one)
        flush(gbs, r)
        send(gbs, gbr, r, 8)

    sum_half(p1r, h1s, h1r, 9, 11)
    for r in range(CHUNKS):
        grad_b(r)
    sum_both(h1s, h1r, g1s, g1r, 11, 12)

    def wait_ga(q, _):
        wait(gar, q, 7)
        return 0

    lax.fori_loop(0, CHUNKS, wait_ga, 0)

    def left(m, _):
        normed = nrm[m]
        p = dot(wt_in[0:256, :], normed, 1, 0)
        tile = pl.ds(pl.multiple_of(m * 128, 128), 128)
        q0 = gar[0, :, :, tile].astype(f32).reshape(CH, 128)
        q1 = gar[1, :, :, tile].astype(f32).reshape(CH, 128)
        q2 = gar[2, :, :, tile].astype(f32).reshape(CH, 128)
        t0, t1 = columns_of(q0, q1)
        ga = jnp.concatenate([t0, t1, q2], axis=1) * pair_mask(m)
        sa = sig(p[0:128])
        gp = jnp.concatenate([ga * p[128:256] * sa * (1.0 - sa), ga * sa], axis=0).astype(bf16)
        gps[m, 0:256, :] = gp
        acc_left[...] += dot(normed, gp, 1, 1)
        return 0

    lax.fori_loop(0, 2 * CHUNKS, left, 0)
    p3s[0] = half_blocks(acc_left[...] * INV)
    send_half(p3s, p3r, 0, 13, HDEV - 1, near, mine)

    def finish(r, _):
        wait(gbr, r, 8)
        for mm in (0, 1):
            m = 2 * r + mm
            at = slice(W * mm, W * mm + W)
            normed = nrm[m]
            p = dot(wt_in[256:512, :], normed, 1, 0)
            gb = gbr[r, :, :, at].astype(f32).reshape(CH, W) * pair_mask(m)
            sb = sig(p[0:128])
            gp = jnp.concatenate([gb * p[128:256] * sb * (1.0 - sb), gb * sb], axis=0).astype(bf16)
            gps[m, 256:512, :] = gp
            acc_right[...] += dot(normed, gp, 1, 1)
        return 0

    lax.fori_loop(0, CHUNKS, finish, 0)
    p2s[0] = blocks(acc_right[...] * INV)
    send(p2s, p2r, 0, 10)
    sum_half(p3r, h3s, h3r, 13, 14)

    def deliver_pair(m):
        rows = pl.ds(2 * m, 2)
        return pltpu.make_async_copy(outv.at[rows], out.at[rows], out_sem.at[m])

    def last(m, _):
        gn = dot(w_in[...], gps[m], 1, 0) + dot(w_ig[...], gl[m], 1, 0)
        zhat, rstd = norm_stats(mid[m].astype(f32))
        acc_norm[...] += lane_sum(gn * zhat)
        gz = norm_grad(gn * cols[:, 4:5], zhat, rstd)
        res = (cott[m].astype(f32) + gz).astype(bf16)
        outv[pl.ds(2 * m, 2)] = dot(sel[...], res, 1, 1).astype(bf16).reshape(2, RES, CH)
        deliver_pair(m).start()
        return 0

    lax.fori_loop(0, 2 * CHUNKS, last, 0)
    sum_both(h3s, h3r, g3s, g3r, 14, 15)

    gains = jnp.concatenate(
        [
            jnp.sum(acc_norm[...].T, axis=0, keepdims=True),
            jnp.sum(acc_mid[...].T, axis=0, keepdims=True),
            jnp.zeros((CG - 2, 128), f32),
        ],
        axis=0,
    )
    g2s[:, 256:384] = (gains * INV).astype(bf16)
    wait(p2r, 0, 10)
    g2s[:, 0:256] = summed(p2r.at[0], DEV).astype(bf16)
    share(g2s, g2r, 16)
    for m in range(2 * CHUNKS):
        deliver_pair(m).wait()

    for ident, ref in ((12, g1r), (15, g3r), (16, g2r)):
        got = ref.at[pl.ds(0, ref.shape[0] - 1)]
        pltpu.make_async_copy(got, got, recv_sem.at[ident, 0]).wait()
    o_all[0:CH, 0:256] = g3r[...].astype(f32).reshape(CH, 256)
    o_all[0:CH, 256:512] = g2r[:, :, 0:256].astype(f32).reshape(CH, 256)
    o_all[0:CH, 512:768] = g1r[...].astype(f32).reshape(CH, 256)
    o_all[CH : CH + CG, 0:128] = summed(g2r.at[:, :, 256:384], DEV)

    for ident, ref, rest in (
        (0, b1r, (0, 1, 2)), (1, a1s, (0, 1, 2)), (2, x1s, (0, 1, 2)), (3, b2s, (0,)),
        (4, a2s, (0, 1, 2)), (5, x2s, (0, 1, 2)), (6, gxs, (0, 1, 2)), (7, gas, (0, 1, 2)),
        (8, gbs, (0, 1, 2)),
        (9, p1s, (0,)), (10, p2s, (0,)), (13, p3s, (0,)),
    ):
        for r in rest:
            sent(ref, r, ident)
    for ident, ref in ((12, g1r), (15, g3r), (16, g2r)):
        gone = ref.at[pl.ds(0, ref.shape[0] - 1)]
        pltpu.make_async_copy(gone, gone, send_sem.at[ident, 0]).wait()
    across(h1s, h1r, 11).wait_send()
    across(h3s, h3r, 14).wait_send()


def deliver(pair_in, all_in, pair_out, proj, gate, final, norm, mid):
    pair_out[...] = pair_in[...]
    proj[...] = all_in[0:CH, 0:512]
    gate[...] = all_in[0:CH, 512:640]
    final[...] = all_in[0:CH, 640:768]
    norm[...] = all_in[CH : CH + 1, 0:128]
    mid[...] = all_in[CH + 1 : CH + 2, 0:128]


def shards(
    pair, cotangent, residue_mask, chain_ids, chain_embed, out_norm_gain, out_proj, out_gate,
    out_mid_gain, out_final, in_norm_gain, in_proj, in_gate, in_mid_gain, in_final,
):
    vm = pl.BlockSpec(memory_space=pltpu.VMEM)
    hbm = pl.BlockSpec(memory_space=pl.ANY)
    v = pltpu.VMEM
    wire = v((CHUNKS, DEV, CG, LANES), bf16)
    half = v((CHUNKS, HDEV, HG, LANES), bf16)
    twice = v((CHUNKS, DEV, HG, LANES), bf16)
    steps = lambda dtype: v((2 * CHUNKS, CH, W), dtype)
    part, part2 = v((1, HDEV, HG, 256), bf16), v((1, DEV, CG, 256), bf16)
    piece, piece2 = v((HG, 256), bf16), v((CG, 384), bf16)
    full, full2 = v((HDEV, HG, 256), bf16), v((DEV, CG, 384), bf16)
    square = v((CH, CH), bf16)
    block = v((ROWS, RES, CH), bf16)
    scratch = (
        [block, block] + [v((1, RES), jnp.int32)] * 2 + [v((2, CH), f32)] + [v((1, CH), f32)] * 4
        + [v((CH, 512), bf16), square, square, v((CH, 512), bf16), square, square]
        + [pltpu.SMEM((1, RES), jnp.int32)] * 2 + [block, v((2 * CHUNKS, 4 * CH, W), bf16)]
        + [v((W, W), bf16), v((CH, 128), f32), v((CH, 128), f32)]
        + [v((4 * CH, CH), bf16), square, square, v((4 * CH, CH), bf16), square, square]
        + [steps(f32), steps(f32), steps(bf16), steps(bf16), steps(bf16), steps(bf16)]
        + [half] * 3 + [wire] * 6 + [part, part2, part, piece, piece2, piece, piece, piece]
        + [twice, half, half] + [wire] * 6 + [part, part2, part, full, full2, full, piece, piece]
        + [v((LANES // 128, DEV * HG, 128), f32), v((LANES // 128, CH, 128), f32)]
        + [v((HG, 256, 256), bf16)]
        + [v((CHUNKS, CG, RES, 128), bf16), v((CG, RES, 256), bf16), v((CHUNKS, CG, 128, 256), bf16)]
        + [v((CH, 256), f32)] * 2 + [v((CH, CH), f32)] * 4
        + [pltpu.SemaphoreType.DMA((17, CHUNKS))] * 2
        + [pltpu.SemaphoreType.DMA((17,)), pltpu.SemaphoreType.DMA((2 * CHUNKS,))]
    )
    mask = residue_mask.reshape(1, RES)
    chain = chain_ids.reshape(1, RES)
    gains = [g.reshape(1, CH) for g in (out_norm_gain, out_mid_gain, in_norm_gain, in_mid_gain)]
    outs = [
        jax.ShapeDtypeStruct((ROWS, RES, CH), bf16),
        jax.ShapeDtypeStruct((CH, 512), f32),
        jax.ShapeDtypeStruct((CH, CH), f32),
        jax.ShapeDtypeStruct((CH, CH), f32),
        jax.ShapeDtypeStruct((1, CH), f32),
        jax.ShapeDtypeStruct((1, CH), f32),
    ]
    params = pltpu.CompilerParams(
        vmem_limit_bytes=60 * 1024 * 1024, collective_id=0, has_side_effects=True
    )
    got = pl.pallas_call(
        kernel,
        out_shape=[outs[0], jax.ShapeDtypeStruct((CH + CG, 768), f32)],
        in_specs=[hbm] * 15,
        out_specs=[hbm, vm],
        scratch_shapes=scratch,
        compiler_params=params,
    )(
        pair, cotangent, mask, chain, chain_embed, *gains,
        out_proj, out_gate, out_final, in_proj, in_gate, in_final,
    )
    got = pl.pallas_call(deliver, out_shape=outs, in_specs=[vm] * 2, out_specs=[vm] * 6)(*got)
    return (*got[:4], got[4].reshape(CH), got[5].reshape(CH))


def solution(mesh):
    whole = P()
    placed = (P("dap", "cplx", None), P("dap", "cplx", None), P("cplx"), P("cplx")) + (whole,) * 11
    return jax.shard_map(
        shards,
        mesh=mesh,
        in_specs=placed,
        out_specs=(
            P("dap", "cplx", None),
            P("cplx", None),
            P("cplx", None),
            P("cplx", None),
            P("cplx"),
            P("cplx"),
        ),
        check_vma=False,
    )
```

```python
import jax
import jax.numpy as jnp
from jax import lax
from jax.experimental import pallas as pl
from jax.experimental.pallas import tpu as pltpu
from jax.sharding import PartitionSpec as P

f32 = jnp.float32
bf16 = jnp.bfloat16

ROWS, RES, CH, DEV = 12, 192, 128, 16
CG = CH // DEV
HDEV = DEV // 2
HG = CH // HDEV
W = 2 * RES
CHUNKS = 3
LANES = 2 * W
EPS = 1e-5
INV = 1.0 / RES
MESH = pl.DeviceIdType.MESH


def dot(a, b, ca, cb):
    return lax.dot_general(a, b, (((ca,), (cb,)), ((), ())), preferred_element_type=f32)


def norm_stats(v):
    mean = jnp.mean(v, axis=0, keepdims=True)
    cent = v - mean
    var = jnp.mean(cent * cent, axis=0, keepdims=True)
    rstd = lax.rsqrt(var + EPS)
    return cent * rstd, rstd


def norm_grad(gh, xhat, rstd):
    return rstd * (
        gh
        - jnp.mean(gh, axis=0, keepdims=True)
        - xhat * jnp.mean(gh * xhat, axis=0, keepdims=True)
    )


def sig(v):
    return jax.nn.sigmoid(v)


def lane_sum(v):
    total = v[:, 0:128]
    for t in range(1, v.shape[1] // 128):
        total = total + v[:, 128 * t : 128 * t + 128]
    return total


def low(rows):
    return lax.broadcasted_iota(jnp.int32, (rows, 128), 1) < 64


def swap(v):
    return pltpu.roll(v, 64, 1)


def selector():
    lane = lax.broadcasted_iota(jnp.int32, (W, W), 1)
    src = lax.broadcasted_iota(jnp.int32, (W, W), 0)
    tail = lane - 256
    first = lane < 256
    i = jnp.where(first, lane >> 7, tail >> 6)
    pos = jnp.where(first, lane & 127, 128 + (tail & 63))
    res = (pos & (DEV - 1)) * ROWS + (pos >> 4)
    return jnp.where(src == i * RES + res, 1.0, 0.0).astype(bf16)


def turn(w):
    return w.astype(f32).T.astype(bf16)


def kernel(
    pair_h, cot_h, mask_h, chain_h, embed_h, gain0_h, gain1_h, gain2_h, gain3_h,
    w_out_h, w_og_h, w_of_h, w_in_h, w_ig_h, w_if_h,
    out, o_all,
    pair, cot, mask_row, chain_row, embed, gain0, gain1, gain2, gain3,
    w_out, w_og, w_of, w_in, w_ig, w_if, mask_s, chain_s, gps, fac, scale, sums,
    sel, vecs, cols, wt_out, wt_og, wt_of, wt_in, wt_ig, wt_if,
    start, gate, mid, nrm, gl, cott,
    b1s, a1s, x1s, b2s, a2s, x2s, gxs, gas, gbs, p1s, p2s, p3s, g1s, g2s, g3s, g4s, h1s, h3s,
    b1r, a1r, x1r, b2r, a2r, x2r, gxr, gar, gbr, p1r, p2r, p3r, g1r, g2r, g3r, g4r, h1r, h3r,
    wide, back, bm, aq, b2, gq, acc_left, acc_right, acc_gate, acc_final, acc_norm, acc_mid,
    send_sem, recv_sem, load_sem,
):
    me = lax.axis_index("dap")
    mx, mz = me // 4, me % 4

    def peer(i):
        k = i // 4
        d = 2 + k - (k // 2) * (2 * k - 1)
        z = (mz // 2 + d // 2) % 2 * 2 + (mz + d) % 2
        return ((mx + 3 - i % 4) % 4) * 4 + z

    mine = mx * 2 + mz % 2

    def seat(to):
        return (to // 4) * 2 + to % 2

    def near(i):
        o = HDEV - 1 - i
        return ((mx + o % 4) % 4) * 4 + (mz // 2) * 2 + (mz + o // 4) % 2

    barrier = pltpu.get_barrier_semaphore()

    def greet(i, _):
        pl.semaphore_signal(barrier, inc=1, device_id={"dap": peer(i)}, device_id_type=MESH)
        return 0

    lax.fori_loop(0, DEV - 1, greet, 0)

    loads = [
        pltpu.make_async_copy(src, dst, load_sem.at[i])
        for i, (src, dst) in enumerate(
            (
                (embed_h, embed), (gain0_h, gain0), (gain1_h, gain1), (gain2_h, gain2),
                (gain3_h, gain3), (w_og_h, w_og), (w_out_h, w_out),
                (mask_h, mask_row), (chain_h, chain_row), (mask_h, mask_s), (chain_h, chain_s),
                (pair_h, pair), (cot_h, cot),
                (w_of_h, w_of), (w_in_h, w_in), (w_ig_h, w_ig), (w_if_h, w_if),
            )
        )
    ]
    for load in loads:
        load.start()

    def send(src, dst, r, ident):
        def one(i, _):
            to = peer(i)
            pltpu.make_async_remote_copy(
                src_ref=src.at[r, to],
                dst_ref=dst.at[r, me],
                send_sem=send_sem.at[ident, r],
                recv_sem=recv_sem.at[ident, r],
                device_id={"dap": to},
                device_id_type=MESH,
            ).start()
            return 0

        lax.fori_loop(0, DEV - 1, one, 0)
        dst[r, me] = src[r, me]

    def send_half(src, dst, r, ident, count, partner, slot):
        def one(i, _):
            to = partner(i)
            pltpu.make_async_remote_copy(
                src_ref=src.at[r, seat(to)],
                dst_ref=dst.at[r, slot],
                send_sem=send_sem.at[ident, r],
                recv_sem=recv_sem.at[ident, r],
                device_id={"dap": to},
                device_id_type=MESH,
            ).start()
            return 0

        lax.fori_loop(0, count, one, 0)
        dst[r, slot] = src[r, mine]

    def share(src, dst, ident):
        def one(i, _):
            pltpu.make_async_remote_copy(
                src_ref=src,
                dst_ref=dst.at[me],
                send_sem=send_sem.at[ident, 0],
                recv_sem=recv_sem.at[ident, 0],
                device_id={"dap": peer(i)},
                device_id_type=MESH,
            ).start()
            return 0

        lax.fori_loop(0, DEV - 1, one, 0)
        dst[me] = src[...]

    def share_half(src, dst, ident):
        def one(i, _):
            pltpu.make_async_remote_copy(
                src_ref=src,
                dst_ref=dst.at[mine],
                send_sem=send_sem.at[ident, 0],
                recv_sem=recv_sem.at[ident, 0],
                device_id={"dap": near(i)},
                device_id_type=MESH,
            ).start()
            return 0

        lax.fori_loop(0, HDEV - 1, one, 0)
        dst[mine] = src[...]

    def across(src, dst, ident):
        return pltpu.make_async_remote_copy(
            src_ref=src,
            dst_ref=dst,
            send_sem=send_sem.at[ident, 0],
            recv_sem=recv_sem.at[ident, 0],
            device_id={"dap": mx * 4 + (mz + 2) % 4},
            device_id_type=MESH,
        )

    def summed(ref, count):
        total = ref[0].astype(f32)
        for k in range(1, count):
            total = total + ref[k].astype(f32)
        return total

    def wait(dst, r, ident):
        blocks = dst.at[r, pl.ds(0, dst.shape[1] - 1)]
        pltpu.make_async_copy(blocks, blocks, recv_sem.at[ident, r]).wait()

    sel[...] = selector()
    vecs[...] = jnp.zeros_like(vecs)
    for load in loads[:11]:
        load.wait()
    vecs[0:2, :] = embed[...]
    vecs[2:3, :] = gain0[...]
    vecs[3:4, :] = gain1[...]
    vecs[4:5, :] = gain2[...]
    vecs[5:6, :] = gain3[...]
    cols[...] = vecs[...].T
    for t in range(4):
        wt_out[128 * t : 128 * t + 128, :] = turn(w_out[:, 128 * t : 128 * t + 128])
    wt_og[...] = turn(w_og[...])

    def by_lane(row_ref):
        wide_row = jnp.broadcast_to(row_ref[...].astype(f32), (16, RES)).astype(bf16)
        return (dot(wide_row, sel[0:RES, :], 1, 0) + dot(wide_row, sel[RES:W, :], 1, 0))[0:1]

    lane = lax.broadcasted_iota(jnp.int32, (1, W), 1)
    second = jnp.where(lane < 256, lane >> 7, (lane - 256) >> 6) == 1
    lane_mask = by_lane(mask_row)
    lane_chain = by_lane(chain_row)

    def row_pair(ref, m):
        at = me * ROWS + 2 * m
        return jnp.where(second, ref[0, at + 1].astype(f32), ref[0, at].astype(f32))

    def pair_mask(m):
        return row_pair(mask_s, m) * lane_mask

    def to_channels(ref, m):
        return dot(ref[pl.ds(2 * m, 2)].reshape(W, CH), sel[...], 0, 0)

    def blocks(v):
        return v.reshape(DEV, CG, v.shape[1]).astype(bf16)

    def half_blocks(v):
        return v.reshape(HDEV, HG, v.shape[1]).astype(bf16)

    loads[11].wait()

    def project(r, _):
        for mm in (0, 1):
            m = 2 * r + mm
            at = slice(W * mm, W * mm + W)
            same = row_pair(chain_s, m) == lane_chain
            st = to_channels(pair, m) + jnp.where(same, cols[:, 1:2], cols[:, 0:1])
            start[m] = st
            xhat, _ = norm_stats(st)
            normed = (xhat * cols[:, 2:3]).astype(bf16)
            p = dot(wt_out[...], normed, 1, 0)
            pm = pair_mask(m)
            b1s[r, :, :, at] = half_blocks(pm * sig(p[256:384]) * p[384:512])
            a1s[r, :, :, at] = half_blocks(pm * sig(p[0:128]) * p[128:256])
            gate[m] = sig(dot(wt_og[...], normed, 1, 0))
        return 0

    project(0, 0)
    pl.semaphore_wait(barrier, DEV - 1)

    def send_b1(r, _):
        send_half(b1s, b1r, r, 0, DEV - 1, peer, me)
        return 0

    def send_a1(r, _):
        send_half(a1s, a1r, r, 1, HDEV - 1, near, mine)
        return 0

    def sent(ref, r, ident):
        blocks_out = ref.at[r, pl.ds(0, ref.shape[1] - 1)]
        pltpu.make_async_copy(blocks_out, blocks_out, send_sem.at[ident, r]).wait()

    send_b1(0, 0)

    def project_and_send(r, _):
        project(r, 0)
        send_b1(r, 0)
        return 0

    lax.fori_loop(1, CHUNKS, project_and_send, 0)
    send_a1(0, 0)

    for load in loads[12:]:
        load.wait()
    for t in range(4):
        wt_in[128 * t : 128 * t + 128, :] = turn(w_in[:, 128 * t : 128 * t + 128])
    wt_of[...] = turn(w_of[...])
    wt_ig[...] = turn(w_ig[...])
    wt_if[...] = turn(w_if[...])

    def turn_cot(m, _):
        cott[m] = to_channels(cot, m).astype(bf16)
        return 0

    lax.fori_loop(0, 2 * CHUNKS, turn_cot, 0)
    bm[:, RES:256, :] = jnp.zeros((HG, 256 - RES, 256), bf16)

    def channels(count, body, width=4):
        def group(g, _):
            for u in range(width):
                body(g * width + u)
            return 0

        lax.fori_loop(0, count // width, group, 0)

    def widen(src, r):
        rows = src.shape[1] * src.shape[2]
        for t in range(LANES // 128):
            tile = src[r, :, :, 128 * t : 128 * t + 128].astype(f32)
            wide[t, 0:rows, :] = tile.reshape(rows, 128)

    def fill_rows(c, put, stride=CG):
        pick = pl.ds(c, DEV, stride=stride)
        lo = low(DEV)
        for mm in (0, 1):
            tail = wide[3 * mm + 2, pick, :]
            put(32 * mm, wide[3 * mm, pick, :], jnp.where(lo, tail, 0.0))
            put(32 * mm + 16, wide[3 * mm + 1, pick, :], jnp.where(lo, swap(tail), 0.0))

    def rows_into(mat, r, c, stride):
        base = r * 64

        def put(row, head, tail):
            at = pl.ds(pl.multiple_of(base + row, 16), 16)
            mat[c, at, 0:128] = head.astype(bf16)
            mat[c, at, 128:256] = tail.astype(bf16)

        fill_rows(c, put, stride)

    def take_rows(src, r, mat):
        widen(src, r)
        count = src.shape[2]

        channels(count, lambda c: rows_into(mat, r, c, count))

    def rows_out(res, c):
        pick = pl.ds(c, DEV, stride=CG)
        lo = low(DEV)
        for mm in (0, 1):
            r = 32 * mm
            back[3 * mm, pick, :] = res[r : r + 16, 0:128]
            back[3 * mm + 1, pick, :] = res[r + 16 : r + 32, 0:128]
            back[3 * mm + 2, pick, :] = jnp.where(
                lo, res[r : r + 16, 128:256], swap(res[r + 16 : r + 32, 128:256])
            )

    def flush(dst, r):
        for t in range(LANES // 128):
            tile = back[t].reshape(dst.shape[1], dst.shape[2], 128)
            dst[r, :, :, 128 * t : 128 * t + 128] = tile.astype(bf16)

    def take_b1(r):
        wait(b1r, r, 0)
        take_rows(b1r, r, bm)

    take_b1(0)
    lax.fori_loop(1, CHUNKS, send_a1, 0)
    take_b1(1)
    take_b1(2)

    def product_out(r, _):
        wait(a1r, r, 1)
        widen(a1r, r)

        def one(c):
            pick = pl.ds(c, HDEV, stride=HG)
            lo = low(HDEV)
            parts = []
            for mm in (0, 1):
                tail = wide[3 * mm + 2, pick, :]
                heads = jnp.concatenate([wide[3 * mm, pick, :], wide[3 * mm + 1, pick, :]], axis=0)
                tails = jnp.concatenate(
                    [jnp.where(lo, tail, 0.0), jnp.where(lo, swap(tail), 0.0)], axis=0
                )
                parts.append(jnp.concatenate([heads, tails], axis=1))
            rows = jnp.concatenate(parts, axis=0).astype(bf16)
            res = dot(rows, bm[c], 1, 1)
            for mm in (0, 1):
                u = 16 * mm
                back[3 * mm, pick, :] = res[u : u + 8, 0:128]
                back[3 * mm + 1, pick, :] = res[u + 8 : u + 16, 0:128]
                back[3 * mm + 2, pick, :] = jnp.where(
                    lo, res[u : u + 8, 128:256], swap(res[u + 8 : u + 16, 128:256])
                )

        channels(HG, one)
        flush(x1s, r)
        send_half(x1s, x1r, r, 2, HDEV - 1, near, mine)
        return 0

    lax.fori_loop(0, CHUNKS, product_out, 0)

    def columns_of(t0, t1):
        lo = low(CH)
        return jnp.where(lo, t0, swap(t1)), jnp.where(lo, swap(t0), t1)

    def middle(r, _):
        wait(x1r, r, 2)
        for mm in (0, 1):
            m = 2 * r + mm
            at = slice(W * mm, W * mm + W)
            xhat, _ = norm_stats(x1r[r, :, :, at].astype(f32).reshape(CH, W))
            y = (xhat * cols[:, 3:4]).astype(bf16)
            md = (start[m] + gate[m] * dot(wt_of[...], y, 1, 0)).astype(bf16)
            mid[m] = md
            zhat, _ = norm_stats(md.astype(f32))
            normed = (zhat * cols[:, 4:5]).astype(bf16)
            nrm[m] = normed
            p = dot(wt_in[...], normed, 1, 0)
            pm = pair_mask(m)
            b2s[r, :, :, at] = blocks(pm * sig(p[256:384]) * p[384:512])
            a = pm * sig(p[0:128]) * p[128:256]
            q0, q1 = columns_of(a[:, 0:128], a[:, 128:256])
            tile = pl.ds(pl.multiple_of(m * 128, 128), 128)
            a2s[0, :, :, tile] = blocks(q0)
            a2s[1, :, :, tile] = blocks(q1)
            a2s[2, :, :, tile] = blocks(a[:, 256:384])
        send(b2s, b2r, r, 3)
        return 0

    lax.fori_loop(0, CHUNKS, middle, 0)
    send(a2s, a2r, 0, 4)

    for r in range(CHUNKS):
        if r > 0:
            sent(b2s, r, 3)
            send(a2s, a2r, r, 4)
        wait(b2r, r, 3)
        take_rows(b2r, r, b2)

    def product_in(q, _):
        wait(a2r, q, 4)
        widen(a2r, q)

        def one(c):
            pick = pl.ds(c, DEV, stride=CG)
            lo = low(DEV)
            parts = []
            for m in range(2 * CHUNKS):
                t = wide[m, pick, :]
                parts.append(jnp.where(lo, t, 0.0).astype(bf16))
                parts.append(jnp.where(lo, swap(t), 0.0).astype(bf16))
            cols_q = jnp.concatenate(parts, axis=0)
            aq[q, c] = cols_q
            rows_out(dot(cols_q, b2[c], 0, 0), c)

        channels(CG, one)
        flush(x2s, q)
        send(x2s, x2r, q, 5)
        return 0

    lax.fori_loop(0, CHUNKS, product_in, 0)

    acc_gate[...] = jnp.zeros_like(acc_gate)
    acc_final[...] = jnp.zeros_like(acc_final)
    acc_mid[...] = jnp.zeros_like(acc_mid)
    acc_left[...] = jnp.zeros_like(acc_left)
    acc_right[...] = jnp.zeros_like(acc_right)
    acc_norm[...] = jnp.zeros_like(acc_norm)

    def values(r, _):
        wait(x2r, r, 5)
        for mm in (0, 1):
            m = 2 * r + mm
            at = slice(W * mm, W * mm + W)
            xhat, rstd = norm_stats(x2r[r, :, :, at].astype(f32).reshape(CH, W))
            gain = cols[:, 5:6]
            y = (xhat * gain).astype(bf16)
            normed = nrm[m]
            ct = cott[m].astype(f32)
            s = sig(dot(wt_ig[...], normed, 1, 0))
            value = dot(wt_if[...], y, 1, 0)
            gv = (ct * s).astype(bf16)
            gy = dot(w_if[...], gv, 1, 0)
            gx = norm_grad(gy * gain, xhat, rstd)
            gxs[r, :, :, at] = blocks(gx)
            glm = (ct * value * s * (1.0 - s)).astype(bf16)
            gl[m] = glm
            acc_final[...] += dot(y, gv, 1, 1)
            acc_gate[...] += dot(normed, glm, 1, 1)
            acc_mid[...] += lane_sum(gy * xhat)
        send(gxs, gxr, r, 6)
        return 0

    lax.fori_loop(0, CHUNKS, values, 0)
    p1s[0, :, :, 0:128] = half_blocks(acc_gate[...] * INV)
    p1s[0, :, :, 128:256] = half_blocks(acc_final[...] * INV)
    send_half(p1s, p1r, 0, 9, HDEV - 1, near, mine)

    def sum_half(src, half_sum, other, ident, next_ident):
        wait(src, 0, ident)
        half_sum[...] = summed(src.at[0], HDEV).astype(bf16)
        across(half_sum, other, next_ident).start()

    def sum_both(half_sum, other, full, result, ident, next_ident):
        across(half_sum, other, ident).wait_recv()
        full[...] = (half_sum[...].astype(f32) + other[...].astype(f32)).astype(bf16)
        share_half(full, result, next_ident)

    def grad_a(q, _):
        wait(gxr, q, 6)
        widen(gxr, q)

        def one(c):
            parts = []

            def put(row, head, tail):
                parts.append(jnp.concatenate([head, tail], axis=1).astype(bf16))

            fill_rows(c, put)
            parts.append(jnp.zeros((64, 256), bf16))
            rows_q = jnp.concatenate(parts, axis=0)
            gq[q, c] = rows_q
            res = dot(b2[c], rows_q, 1, 1)
            pick = pl.ds(c, DEV, stride=CG)
            lo = low(DEV)
            for m in range(2 * CHUNKS):
                back[m, pick, :] = jnp.where(
                    lo, res[32 * m : 32 * m + 16], swap(res[32 * m + 16 : 32 * m + 32])
                )

        channels(CG, one)
        flush(gas, q)
        send(gas, gar, q, 7)
        return 0

    lax.fori_loop(0, CHUNKS, grad_a, 0)

    def grad_b(r):
        rows = pl.ds(pl.multiple_of(r * 64, 64), 64)

        def one(c):
            res = dot(aq[0, c, rows, :], gq[0, c], 1, 0)
            for q in (1, 2):
                res = res + dot(aq[q, c, rows, :], gq[q, c], 1, 0)
            rows_out(res, c)

        channels(CG, one)
        flush(gbs, r)
        send(gbs, gbr, r, 8)

    for r in range(CHUNKS):
        grad_b(r)

    def prepare(m, _):
        p = dot(wt_in[...], nrm[m], 1, 0)
        pm = pair_mask(m)
        for k in (0, 256):
            s = sig(p[k : k + 128])
            fac[m, k : k + 128, :] = pm * p[k + 128 : k + 256] * s * (1.0 - s)
            fac[m, k + 128 : k + 256, :] = pm * s
        zhat, rstd = norm_stats(mid[m].astype(f32))
        start[m] = zhat
        scale[m] = jnp.broadcast_to(rstd, (CG, W))
        gate[m] = dot(w_ig[...], gl[m], 1, 0)
        return 0

    lax.fori_loop(0, 2 * CHUNKS, prepare, 0)
    sums[1:2, :] = jnp.sum(acc_mid[...].T, axis=0, keepdims=True)
    sum_half(p1r, h1s, h1r, 9, 11)

    def wait_ga(q, _):
        wait(gar, q, 7)
        return 0

    lax.fori_loop(0, CHUNKS, wait_ga, 0)

    def left(m, _):
        tile = pl.ds(pl.multiple_of(m * 128, 128), 128)
        q0 = gar[0, :, :, tile].astype(f32).reshape(CH, 128)
        q1 = gar[1, :, :, tile].astype(f32).reshape(CH, 128)
        q2 = gar[2, :, :, tile].astype(f32).reshape(CH, 128)
        t0, t1 = columns_of(q0, q1)
        ga = jnp.concatenate([t0, t1, q2], axis=1)
        gp = jnp.concatenate([ga * fac[m, 0:128, :], ga * fac[m, 128:256, :]], axis=0).astype(bf16)
        gps[m, 0:256, :] = gp
        acc_left[...] += dot(nrm[m], gp, 1, 1)
        return 0

    lax.fori_loop(0, 2 * CHUNKS, left, 0)
    p3s[0] = half_blocks(acc_left[...] * INV)
    send_half(p3s, p3r, 0, 13, HDEV - 1, near, mine)

    def finish(r, _):
        wait(gbr, r, 8)
        for mm in (0, 1):
            m = 2 * r + mm
            at = slice(W * mm, W * mm + W)
            gb = gbr[r, :, :, at].astype(f32).reshape(CH, W)
            gp = jnp.concatenate(
                [gb * fac[m, 256:384, :], gb * fac[m, 384:512, :]], axis=0
            ).astype(bf16)
            gps[m, 256:512, :] = gp
            acc_right[...] += dot(nrm[m], gp, 1, 1)
        return 0

    lax.fori_loop(0, CHUNKS, finish, 0)
    p2s[0] = blocks(acc_right[...] * INV)
    send(p2s, p2r, 0, 10)
    sum_both(h1s, h1r, g1s, g1r, 11, 12)

    def last(m, _):
        gn = dot(w_in[...], gps[m], 1, 0) + gate[m]
        zhat, rstd = start[m], scale[m, 0:1, :]
        acc_norm[...] += lane_sum(gn * zhat)
        gz = norm_grad(gn * cols[:, 4:5], zhat, rstd)
        res = (cott[m].astype(f32) + gz).astype(bf16)
        out[pl.ds(2 * m, 2)] = dot(sel[...], res, 1, 1).astype(bf16).reshape(2, RES, CH)
        return 0

    lax.fori_loop(0, CHUNKS, last, 0)
    sum_half(p3r, h3s, h3r, 13, 14)
    lax.fori_loop(CHUNKS, 2 * CHUNKS, last, 0)

    sums[0:1, :] = jnp.sum(acc_norm[...].T, axis=0, keepdims=True)
    g4s[...] = (sums[0:2, :] * INV).astype(bf16)
    share(g4s, g4r, 17)
    wait(p2r, 0, 10)
    g2s[...] = summed(p2r.at[0], DEV).astype(bf16)
    share(g2s, g2r, 16)
    sum_both(h3s, h3r, g3s, g3r, 14, 15)

    for ident, ref in ((12, g1r), (17, g4r), (15, g3r), (16, g2r)):
        got = ref.at[pl.ds(0, ref.shape[0] - 1)]
        pltpu.make_async_copy(got, got, recv_sem.at[ident, 0]).wait()
    o_all[0:CH, 0:256] = g3r[...].astype(f32).reshape(CH, 256)
    o_all[0:CH, 256:512] = g2r[...].astype(f32).reshape(CH, 256)
    o_all[0:CH, 512:768] = g1r[...].astype(f32).reshape(CH, 256)
    o_all[CH : CH + 2, 0:128] = summed(g4r, DEV)

    for ident, ref, rest in (
        (0, b1r, (0, 1, 2)), (1, a1s, (0, 1, 2)), (2, x1s, (0, 1, 2)), (3, b2s, (0,)),
        (4, a2s, (0, 1, 2)), (5, x2s, (0, 1, 2)), (6, gxs, (0, 1, 2)), (7, gas, (0, 1, 2)),
        (8, gbs, (0, 1, 2)),
        (9, p1s, (0,)), (10, p2s, (0,)), (13, p3s, (0,)),
    ):
        for r in rest:
            sent(ref, r, ident)
    for ident, ref in ((12, g1r), (17, g4r), (15, g3r), (16, g2r)):
        gone = ref.at[pl.ds(0, ref.shape[0] - 1)]
        pltpu.make_async_copy(gone, gone, send_sem.at[ident, 0]).wait()
    across(h1s, h1r, 11).wait_send()
    across(h3s, h3r, 14).wait_send()


def deliver(pair_in, all_in, pair_out, proj, gate, final, norm, mid, sem):
    copies = [
        pltpu.make_async_copy(src, dst, sem.at[i])
        for i, (src, dst) in enumerate(
            (
                (pair_in, pair_out),
                (all_in.at[0:CH, 0:512], proj),
                (all_in.at[0:CH, 512:640], gate),
                (all_in.at[0:CH, 640:768], final),
            )
        )
    ]
    for copy in copies:
        copy.start()
    norm[...] = all_in[CH : CH + 1, 0:128]
    mid[...] = all_in[CH + 1 : CH + 2, 0:128]
    for copy in copies:
        copy.wait()


def shards(
    pair, cotangent, residue_mask, chain_ids, chain_embed, out_norm_gain, out_proj, out_gate,
    out_mid_gain, out_final, in_norm_gain, in_proj, in_gate, in_mid_gain, in_final,
):
    vm = pl.BlockSpec(memory_space=pltpu.VMEM)
    hbm = pl.BlockSpec(memory_space=pl.ANY)
    v = pltpu.VMEM
    wire = v((CHUNKS, DEV, CG, LANES), bf16)
    half = v((CHUNKS, HDEV, HG, LANES), bf16)
    twice = v((CHUNKS, DEV, HG, LANES), bf16)
    steps = lambda dtype: v((2 * CHUNKS, CH, W), dtype)
    part, part2 = v((1, HDEV, HG, 256), bf16), v((1, DEV, CG, 256), bf16)
    piece, piece2, row = v((HG, 256), bf16), v((CG, 256), bf16), v((2, CH), bf16)
    full, full2 = v((HDEV, HG, 256), bf16), v((DEV, CG, 256), bf16)
    rows = v((DEV, 2, CH), bf16)
    square = v((CH, CH), bf16)
    block = v((ROWS, RES, CH), bf16)
    scratch = (
        [block, block] + [v((1, RES), jnp.int32)] * 2 + [v((2, CH), f32)] + [v((1, CH), f32)] * 4
        + [v((CH, 512), bf16), square, square, v((CH, 512), bf16), square, square]
        + [pltpu.SMEM((1, RES), jnp.int32)] * 2 + [v((2 * CHUNKS, 4 * CH, W), bf16)]
        + [v((2 * CHUNKS, 4 * CH, W), f32), v((2 * CHUNKS, CG, W), f32), v((CG, CH), f32)]
        + [v((W, W), bf16), v((CH, 128), f32), v((CH, 128), f32)]
        + [v((4 * CH, CH), bf16), square, square, v((4 * CH, CH), bf16), square, square]
        + [steps(f32), steps(f32), steps(bf16), steps(bf16), steps(bf16), steps(bf16)]
        + [half] * 3 + [wire] * 6 + [part, part2, part, piece, piece2, piece, row, piece, piece]
        + [twice, half, half] + [wire] * 6 + [part, part2, part, full, full2, full, rows, piece, piece]
        + [v((LANES // 128, DEV * HG, 128), f32), v((LANES // 128, CH, 128), f32)]
        + [v((HG, 256, 256), bf16)]
        + [v((CHUNKS, CG, RES, 128), bf16), v((CG, RES, 256), bf16), v((CHUNKS, CG, 128, 256), bf16)]
        + [v((CH, 256), f32)] * 2 + [v((CH, CH), f32)] * 4
        + [pltpu.SemaphoreType.DMA((18, CHUNKS))] * 2
        + [pltpu.SemaphoreType.DMA((17,))]
    )
    mask = residue_mask.reshape(1, RES)
    chain = chain_ids.reshape(1, RES)
    gains = [g.reshape(1, CH) for g in (out_norm_gain, out_mid_gain, in_norm_gain, in_mid_gain)]
    outs = [
        jax.ShapeDtypeStruct((ROWS, RES, CH), bf16),
        jax.ShapeDtypeStruct((CH, 512), f32),
        jax.ShapeDtypeStruct((CH, CH), f32),
        jax.ShapeDtypeStruct((CH, CH), f32),
        jax.ShapeDtypeStruct((1, CH), f32),
        jax.ShapeDtypeStruct((1, CH), f32),
    ]
    params = pltpu.CompilerParams(
        vmem_limit_bytes=60 * 1024 * 1024, collective_id=0, has_side_effects=True
    )
    got = pl.pallas_call(
        kernel,
        out_shape=[pltpu.VMEM((ROWS, RES, CH), bf16), pltpu.VMEM((CH + CG, 768), f32)],
        in_specs=[hbm] * 15,
        out_specs=[vm, vm],
        scratch_shapes=scratch,
        compiler_params=params,
    )(
        pair, cotangent, mask, chain, chain_embed, *gains,
        out_proj, out_gate, out_final, in_proj, in_gate, in_final,
    )
    got = [pltpu.with_memory_space_constraint(g, pltpu.VMEM) for g in got]
    got = pl.pallas_call(
        deliver,
        out_shape=outs,
        in_specs=[vm] * 2,
        out_specs=[hbm] * 4 + [vm] * 2,
        scratch_shapes=[pltpu.SemaphoreType.DMA((4,))],
    )(*got)
    return (*got[:4], got[4].reshape(CH), got[5].reshape(CH))


def solution(mesh):
    whole = P()
    placed = (P("dap", "cplx", None), P("dap", "cplx", None), P("cplx"), P("cplx")) + (whole,) * 11
    return jax.shard_map(
        shards,
        mesh=mesh,
        in_specs=placed,
        out_specs=(
            P("dap", "cplx", None),
            P("cplx", None),
            P("cplx", None),
            P("cplx", None),
            P("cplx"),
            P("cplx"),
        ),
        check_vma=False,
    )
```

```python
import jax
import jax.numpy as jnp
from jax import lax
from jax.experimental import pallas as pl
from jax.experimental.pallas import tpu as pltpu
from jax.sharding import PartitionSpec as P

f32 = jnp.float32
bf16 = jnp.bfloat16

ROWS, RES, CH, DEV = 12, 192, 128, 16
CG = CH // DEV
HDEV = DEV // 2
HG = CH // HDEV
W = 2 * RES
CHUNKS = 3
LANES = 2 * W
EPS = 1e-5
INV = 1.0 / RES
MESH = pl.DeviceIdType.MESH


def dot(a, b, ca, cb):
    return lax.dot_general(a, b, (((ca,), (cb,)), ((), ())), preferred_element_type=f32)


def norm_stats(v):
    mean = jnp.mean(v, axis=0, keepdims=True)
    cent = v - mean
    var = jnp.mean(cent * cent, axis=0, keepdims=True)
    rstd = lax.rsqrt(var + EPS)
    return cent * rstd, rstd


def norm_grad(gh, xhat, rstd):
    return rstd * (
        gh
        - jnp.mean(gh, axis=0, keepdims=True)
        - xhat * jnp.mean(gh * xhat, axis=0, keepdims=True)
    )


def sig(v):
    return jax.nn.sigmoid(v)


def lane_sum(v):
    total = v[:, 0:128]
    for t in range(1, v.shape[1] // 128):
        total = total + v[:, 128 * t : 128 * t + 128]
    return total


def low(rows):
    return lax.broadcasted_iota(jnp.int32, (rows, 128), 1) < 64


def swap(v):
    return pltpu.roll(v, 64, 1)


def selector():
    lane = lax.broadcasted_iota(jnp.int32, (W, W), 1)
    src = lax.broadcasted_iota(jnp.int32, (W, W), 0)
    tail = lane - 256
    first = lane < 256
    i = jnp.where(first, lane >> 7, tail >> 6)
    pos = jnp.where(first, lane & 127, 128 + (tail & 63))
    res = (pos & (DEV - 1)) * ROWS + (pos >> 4)
    return jnp.where(src == i * RES + res, 1.0, 0.0).astype(bf16)


def turn(w):
    return w.astype(f32).T.astype(bf16)


def kernel(
    pair_h, cot_h, mask_h, chain_h, embed_h, gain0_h, gain1_h, gain2_h, gain3_h,
    w_out_h, w_og_h, w_of_h, w_in_h, w_ig_h, w_if_h,
    out, o_all,
    pair, cot, mask_row, chain_row, embed, gain0, gain1, gain2, gain3,
    w_out, w_og, w_of, w_in, w_ig, w_if, mask_s, chain_s, gps, fac, scale, sums,
    sel, vecs, cols, wt_out, wt_og, wt_of, wt_in, wt_ig, wt_if,
    start, gate, mid, nrm, gl, cott,
    b1s, a1s, x1s, b2s, a2s, x2s, gxs, gas, gbs, p1s, p2s, p3s, g1s, g2s, g3s, g4s, h1s, h3s,
    b1r, a1r, x1r, b2r, a2r, x2r, gxr, gar, gbr, p1r, p2r, p3r, g1r, g2r, g3r, g4r, h1r, h3r,
    wide, back, bm, aq, b2, gq, acc_left, acc_right, acc_gate, acc_final, acc_norm, acc_mid,
    send_sem, recv_sem, load_sem,
):
    me = lax.axis_index("dap")
    mx, mz = me // 4, me % 4

    def peer(i):
        k = i // 4
        d = 2 + k - (k // 2) * (2 * k - 1)
        z = (mz // 2 + d // 2) % 2 * 2 + (mz + d) % 2
        return ((mx + 3 - i % 4) % 4) * 4 + z

    mine = mx * 2 + mz % 2

    def seat(to):
        return (to // 4) * 2 + to % 2

    def near(i):
        o = HDEV - 1 - i
        return ((mx + o % 4) % 4) * 4 + (mz // 2) * 2 + (mz + o // 4) % 2

    barrier = pltpu.get_barrier_semaphore()

    def greet(i, _):
        pl.semaphore_signal(barrier, inc=1, device_id={"dap": peer(i)}, device_id_type=MESH)
        return 0

    lax.fori_loop(0, DEV - 1, greet, 0)

    loads = [
        pltpu.make_async_copy(src, dst, load_sem.at[i])
        for i, (src, dst) in enumerate(
            (
                (embed_h, embed), (gain0_h, gain0), (gain1_h, gain1), (gain2_h, gain2),
                (gain3_h, gain3), (w_og_h, w_og), (w_out_h, w_out),
                (mask_h, mask_row), (chain_h, chain_row), (mask_h, mask_s), (chain_h, chain_s),
                (pair_h, pair), (cot_h, cot),
                (w_of_h, w_of), (w_in_h, w_in), (w_ig_h, w_ig), (w_if_h, w_if),
            )
        )
    ]
    for load in loads:
        load.start()

    def send(src, dst, r, ident):
        def one(i, _):
            to = peer(i)
            pltpu.make_async_remote_copy(
                src_ref=src.at[r, to],
                dst_ref=dst.at[r, me],
                send_sem=send_sem.at[ident, r],
                recv_sem=recv_sem.at[ident, r],
                device_id={"dap": to},
                device_id_type=MESH,
            ).start()
            return 0

        lax.fori_loop(0, DEV - 1, one, 0)
        dst[r, me] = src[r, me]

    def send_half(src, dst, r, ident, count, partner, slot):
        def one(i, _):
            to = partner(i)
            pltpu.make_async_remote_copy(
                src_ref=src.at[r, seat(to)],
                dst_ref=dst.at[r, slot],
                send_sem=send_sem.at[ident, r],
                recv_sem=recv_sem.at[ident, r],
                device_id={"dap": to},
                device_id_type=MESH,
            ).start()
            return 0

        lax.fori_loop(0, count, one, 0)
        dst[r, slot] = src[r, mine]

    def share(src, dst, ident):
        def one(i, _):
            pltpu.make_async_remote_copy(
                src_ref=src,
                dst_ref=dst.at[me],
                send_sem=send_sem.at[ident, 0],
                recv_sem=recv_sem.at[ident, 0],
                device_id={"dap": peer(i)},
                device_id_type=MESH,
            ).start()
            return 0

        lax.fori_loop(0, DEV - 1, one, 0)
        dst[me] = src[...]

    def share_half(src, dst, ident):
        def one(i, _):
            pltpu.make_async_remote_copy(
                src_ref=src,
                dst_ref=dst.at[mine],
                send_sem=send_sem.at[ident, 0],
                recv_sem=recv_sem.at[ident, 0],
                device_id={"dap": near(i)},
                device_id_type=MESH,
            ).start()
            return 0

        lax.fori_loop(0, HDEV - 1, one, 0)
        dst[mine] = src[...]

    def across(src, dst, ident):
        return pltpu.make_async_remote_copy(
            src_ref=src,
            dst_ref=dst,
            send_sem=send_sem.at[ident, 0],
            recv_sem=recv_sem.at[ident, 0],
            device_id={"dap": mx * 4 + (mz + 2) % 4},
            device_id_type=MESH,
        )

    def summed(ref, count):
        total = ref[0].astype(f32)
        for k in range(1, count):
            total = total + ref[k].astype(f32)
        return total

    def wait(dst, r, ident):
        blocks = dst.at[r, pl.ds(0, dst.shape[1] - 1)]
        pltpu.make_async_copy(blocks, blocks, recv_sem.at[ident, r]).wait()

    sel[...] = selector()
    vecs[...] = jnp.zeros_like(vecs)
    for load in loads[:11]:
        load.wait()
    vecs[0:2, :] = embed[...]
    vecs[2:3, :] = gain0[...]
    vecs[3:4, :] = gain1[...]
    vecs[4:5, :] = gain2[...]
    vecs[5:6, :] = gain3[...]
    cols[...] = vecs[...].T
    for t in range(4):
        wt_out[128 * t : 128 * t + 128, :] = turn(w_out[:, 128 * t : 128 * t + 128])
    wt_og[...] = turn(w_og[...])

    def by_lane(row_ref):
        wide_row = jnp.broadcast_to(row_ref[...].astype(f32), (16, RES)).astype(bf16)
        return (dot(wide_row, sel[0:RES, :], 1, 0) + dot(wide_row, sel[RES:W, :], 1, 0))[0:1]

    lane = lax.broadcasted_iota(jnp.int32, (1, W), 1)
    second = jnp.where(lane < 256, lane >> 7, (lane - 256) >> 6) == 1
    lane_mask = by_lane(mask_row)
    lane_chain = by_lane(chain_row)

    def row_pair(ref, m):
        at = me * ROWS + 2 * m
        return jnp.where(second, ref[0, at + 1].astype(f32), ref[0, at].astype(f32))

    def pair_mask(m):
        return row_pair(mask_s, m) * lane_mask

    def to_channels(ref, m):
        return dot(ref[pl.ds(2 * m, 2)].reshape(W, CH), sel[...], 0, 0)

    def blocks(v):
        return v.reshape(DEV, CG, v.shape[1]).astype(bf16)

    def half_blocks(v):
        return v.reshape(HDEV, HG, v.shape[1]).astype(bf16)

    loads[11].wait()

    def project(r, _):
        for mm in (0, 1):
            m = 2 * r + mm
            at = slice(W * mm, W * mm + W)
            same = row_pair(chain_s, m) == lane_chain
            st = to_channels(pair, m) + jnp.where(same, cols[:, 1:2], cols[:, 0:1])
            start[m] = st
            xhat, _ = norm_stats(st)
            normed = (xhat * cols[:, 2:3]).astype(bf16)
            p = dot(wt_out[...], normed, 1, 0)
            pm = pair_mask(m)
            b1s[r, :, :, at] = half_blocks(pm * sig(p[256:384]) * p[384:512])
            a1s[r, :, :, at] = half_blocks(pm * sig(p[0:128]) * p[128:256])
            gate[m] = sig(dot(wt_og[...], normed, 1, 0))
        return 0

    lax.fori_loop(0, 2, project, 0)
    pl.semaphore_wait(barrier, DEV - 1)

    def send_b1(r, _):
        send_half(b1s, b1r, r, 0, DEV - 1, peer, me)
        return 0

    def send_a1(r, _):
        send_half(a1s, a1r, r, 1, HDEV - 1, near, mine)
        return 0

    def sent(ref, r, ident):
        blocks_out = ref.at[r, pl.ds(0, ref.shape[1] - 1)]
        pltpu.make_async_copy(blocks_out, blocks_out, send_sem.at[ident, r]).wait()

    lax.fori_loop(0, 2, send_b1, 0)
    project(2, 0)
    send_b1(2, 0)
    send_a1(0, 0)

    for load in loads[12:]:
        load.wait()
    for t in range(4):
        wt_in[128 * t : 128 * t + 128, :] = turn(w_in[:, 128 * t : 128 * t + 128])
    wt_of[...] = turn(w_of[...])
    wt_ig[...] = turn(w_ig[...])
    wt_if[...] = turn(w_if[...])

    def turn_cot(m, _):
        cott[m] = to_channels(cot, m).astype(bf16)
        return 0

    lax.fori_loop(0, 2 * CHUNKS, turn_cot, 0)
    bm[:, RES:256, :] = jnp.zeros((HG, 256 - RES, 256), bf16)

    def channels(count, body, width=4):
        def group(g, _):
            for u in range(width):
                body(g * width + u)
            return 0

        lax.fori_loop(0, count // width, group, 0)

    def widen(src, r):
        rows = src.shape[1] * src.shape[2]
        for t in range(LANES // 128):
            tile = src[r, :, :, 128 * t : 128 * t + 128].astype(f32)
            wide[t, 0:rows, :] = tile.reshape(rows, 128)

    def fill_rows(c, put, stride=CG):
        pick = pl.ds(c, DEV, stride=stride)
        lo = low(DEV)
        for mm in (0, 1):
            tail = wide[3 * mm + 2, pick, :]
            put(32 * mm, wide[3 * mm, pick, :], jnp.where(lo, tail, 0.0))
            put(32 * mm + 16, wide[3 * mm + 1, pick, :], jnp.where(lo, swap(tail), 0.0))

    def rows_into(mat, r, c, stride):
        base = r * 64

        def put(row, head, tail):
            at = pl.ds(pl.multiple_of(base + row, 16), 16)
            mat[c, at, 0:128] = head.astype(bf16)
            mat[c, at, 128:256] = tail.astype(bf16)

        fill_rows(c, put, stride)

    def take_rows(src, r, mat):
        widen(src, r)
        count = src.shape[2]

        channels(count, lambda c: rows_into(mat, r, c, count))

    def rows_out(res, c):
        pick = pl.ds(c, DEV, stride=CG)
        lo = low(DEV)
        for mm in (0, 1):
            r = 32 * mm
            back[3 * mm, pick, :] = res[r : r + 16, 0:128]
            back[3 * mm + 1, pick, :] = res[r + 16 : r + 32, 0:128]
            back[3 * mm + 2, pick, :] = jnp.where(
                lo, res[r : r + 16, 128:256], swap(res[r + 16 : r + 32, 128:256])
            )

    def flush(dst, r):
        for t in range(LANES // 128):
            tile = back[t].reshape(dst.shape[1], dst.shape[2], 128)
            dst[r, :, :, 128 * t : 128 * t + 128] = tile.astype(bf16)

    def take_b1(r):
        wait(b1r, r, 0)
        take_rows(b1r, r, bm)

    take_b1(0)
    lax.fori_loop(1, CHUNKS, send_a1, 0)
    take_b1(1)
    take_b1(2)

    def product_out(r, _):
        wait(a1r, r, 1)
        widen(a1r, r)

        def one(c):
            pick = pl.ds(c, HDEV, stride=HG)
            lo = low(HDEV)
            parts = []
            for mm in (0, 1):
                tail = wide[3 * mm + 2, pick, :]
                heads = jnp.concatenate([wide[3 * mm, pick, :], wide[3 * mm + 1, pick, :]], axis=0)
                tails = jnp.concatenate(
                    [jnp.where(lo, tail, 0.0), jnp.where(lo, swap(tail), 0.0)], axis=0
                )
                parts.append(jnp.concatenate([heads, tails], axis=1))
            rows = jnp.concatenate(parts, axis=0).astype(bf16)
            res = dot(rows, bm[c], 1, 1)
            for mm in (0, 1):
                u = 16 * mm
                back[3 * mm, pick, :] = res[u : u + 8, 0:128]
                back[3 * mm + 1, pick, :] = res[u + 8 : u + 16, 0:128]
                back[3 * mm + 2, pick, :] = jnp.where(
                    lo, res[u : u + 8, 128:256], swap(res[u + 8 : u + 16, 128:256])
                )

        channels(HG, one, 16)
        flush(x1s, r)
        send_half(x1s, x1r, r, 2, HDEV - 1, near, mine)
        return 0

    lax.fori_loop(0, CHUNKS, product_out, 0)

    def columns_of(t0, t1):
        lo = low(CH)
        return jnp.where(lo, t0, swap(t1)), jnp.where(lo, swap(t0), t1)

    def middle(r, _):
        wait(x1r, r, 2)
        for mm in (0, 1):
            m = 2 * r + mm
            at = slice(W * mm, W * mm + W)
            xhat, _ = norm_stats(x1r[r, :, :, at].astype(f32).reshape(CH, W))
            y = (xhat * cols[:, 3:4]).astype(bf16)
            md = (start[m] + gate[m] * dot(wt_of[...], y, 1, 0)).astype(bf16)
            mid[m] = md
            zhat, _ = norm_stats(md.astype(f32))
            normed = (zhat * cols[:, 4:5]).astype(bf16)
            nrm[m] = normed
            p = dot(wt_in[...], normed, 1, 0)
            pm = pair_mask(m)
            b2s[r, :, :, at] = blocks(pm * sig(p[256:384]) * p[384:512])
            a = pm * sig(p[0:128]) * p[128:256]
            q0, q1 = columns_of(a[:, 0:128], a[:, 128:256])
            tile = pl.ds(pl.multiple_of(m * 128, 128), 128)
            a2s[0, :, :, tile] = blocks(q0)
            a2s[1, :, :, tile] = blocks(q1)
            a2s[2, :, :, tile] = blocks(a[:, 256:384])
        send(b2s, b2r, r, 3)
        return 0

    lax.fori_loop(0, CHUNKS, middle, 0)
    send(a2s, a2r, 0, 4)

    for r in range(CHUNKS):
        if r > 0:
            sent(b2s, r, 3)
            send(a2s, a2r, r, 4)
        wait(b2r, r, 3)
        take_rows(b2r, r, b2)

    def product_in(q, _):
        wait(a2r, q, 4)
        widen(a2r, q)

        def one(c):
            pick = pl.ds(c, DEV, stride=CG)
            lo = low(DEV)
            parts = []
            for m in range(2 * CHUNKS):
                t = wide[m, pick, :]
                parts.append(jnp.where(lo, t, 0.0).astype(bf16))
                parts.append(jnp.where(lo, swap(t), 0.0).astype(bf16))
            cols_q = jnp.concatenate(parts, axis=0)
            aq[q, c] = cols_q
            rows_out(dot(cols_q, b2[c], 0, 0), c)

        channels(CG, one)
        flush(x2s, q)
        send(x2s, x2r, q, 5)
        return 0

    lax.fori_loop(0, CHUNKS, product_in, 0)

    acc_gate[...] = jnp.zeros_like(acc_gate)
    acc_final[...] = jnp.zeros_like(acc_final)
    acc_mid[...] = jnp.zeros_like(acc_mid)
    acc_left[...] = jnp.zeros_like(acc_left)
    acc_right[...] = jnp.zeros_like(acc_right)
    acc_norm[...] = jnp.zeros_like(acc_norm)

    def values(r, _):
        wait(x2r, r, 5)
        for mm in (0, 1):
            m = 2 * r + mm
            at = slice(W * mm, W * mm + W)
            xhat, rstd = norm_stats(x2r[r, :, :, at].astype(f32).reshape(CH, W))
            gain = cols[:, 5:6]
            y = (xhat * gain).astype(bf16)
            normed = nrm[m]
            ct = cott[m].astype(f32)
            s = sig(dot(wt_ig[...], normed, 1, 0))
            value = dot(wt_if[...], y, 1, 0)
            gv = (ct * s).astype(bf16)
            gy = dot(w_if[...], gv, 1, 0)
            gx = norm_grad(gy * gain, xhat, rstd)
            gxs[r, :, :, at] = blocks(gx)
            glm = (ct * value * s * (1.0 - s)).astype(bf16)
            gl[m] = glm
            acc_final[...] += dot(y, gv, 1, 1)
            acc_gate[...] += dot(normed, glm, 1, 1)
            acc_mid[...] += lane_sum(gy * xhat)
        send(gxs, gxr, r, 6)
        return 0

    lax.fori_loop(0, CHUNKS, values, 0)
    p1s[0, :, :, 0:128] = half_blocks(acc_gate[...] * INV)
    p1s[0, :, :, 128:256] = half_blocks(acc_final[...] * INV)
    send_half(p1s, p1r, 0, 9, HDEV - 1, near, mine)

    def sum_half(src, half_sum, other, ident, next_ident):
        wait(src, 0, ident)
        half_sum[...] = summed(src.at[0], HDEV).astype(bf16)
        across(half_sum, other, next_ident).start()

    def sum_both(half_sum, other, full, result, ident, next_ident):
        across(half_sum, other, ident).wait_recv()
        full[...] = (half_sum[...].astype(f32) + other[...].astype(f32)).astype(bf16)
        share_half(full, result, next_ident)

    def grad_a(q, _):
        wait(gxr, q, 6)
        widen(gxr, q)

        def one(c):
            parts = []

            def put(row, head, tail):
                parts.append(jnp.concatenate([head, tail], axis=1).astype(bf16))

            fill_rows(c, put)
            parts.append(jnp.zeros((64, 256), bf16))
            rows_q = jnp.concatenate(parts, axis=0)
            gq[q, c] = rows_q
            res = dot(b2[c], rows_q, 1, 1)
            pick = pl.ds(c, DEV, stride=CG)
            lo = low(DEV)
            for m in range(2 * CHUNKS):
                back[m, pick, :] = jnp.where(
                    lo, res[32 * m : 32 * m + 16], swap(res[32 * m + 16 : 32 * m + 32])
                )

        channels(CG, one)
        flush(gas, q)
        send(gas, gar, q, 7)
        return 0

    lax.fori_loop(0, CHUNKS, grad_a, 0)

    def grad_b(r):
        rows = pl.ds(pl.multiple_of(r * 64, 64), 64)

        def one(c):
            res = dot(aq[0, c, rows, :], gq[0, c], 1, 0)
            for q in (1, 2):
                res = res + dot(aq[q, c, rows, :], gq[q, c], 1, 0)
            rows_out(res, c)

        channels(CG, one)
        flush(gbs, r)
        send(gbs, gbr, r, 8)

    for r in range(CHUNKS):
        grad_b(r)

    def prepare(m, _):
        p = dot(wt_in[...], nrm[m], 1, 0)
        pm = pair_mask(m)
        for k in (0, 256):
            s = sig(p[k : k + 128])
            fac[m, k : k + 128, :] = pm * p[k + 128 : k + 256] * s * (1.0 - s)
            fac[m, k + 128 : k + 256, :] = pm * s
        zhat, rstd = norm_stats(mid[m].astype(f32))
        start[m] = zhat
        scale[m] = jnp.broadcast_to(rstd, (CG, W))
        gate[m] = dot(w_ig[...], gl[m], 1, 0)
        return 0

    lax.fori_loop(0, 2 * CHUNKS, prepare, 0)
    sums[1:2, :] = jnp.sum(acc_mid[...].T, axis=0, keepdims=True)
    sum_half(p1r, h1s, h1r, 9, 11)

    def wait_ga(q, _):
        wait(gar, q, 7)
        return 0

    lax.fori_loop(0, CHUNKS, wait_ga, 0)

    def left(m, _):
        tile = pl.ds(pl.multiple_of(m * 128, 128), 128)
        q0 = gar[0, :, :, tile].astype(f32).reshape(CH, 128)
        q1 = gar[1, :, :, tile].astype(f32).reshape(CH, 128)
        q2 = gar[2, :, :, tile].astype(f32).reshape(CH, 128)
        t0, t1 = columns_of(q0, q1)
        ga = jnp.concatenate([t0, t1, q2], axis=1)
        gp = jnp.concatenate([ga * fac[m, 0:128, :], ga * fac[m, 128:256, :]], axis=0).astype(bf16)
        gps[m, 0:256, :] = gp
        acc_left[...] += dot(nrm[m], gp, 1, 1)
        return 0

    lax.fori_loop(0, 2 * CHUNKS, left, 0)
    p3s[0] = half_blocks(acc_left[...] * INV)
    send_half(p3s, p3r, 0, 13, HDEV - 1, near, mine)

    def finish(r, _):
        wait(gbr, r, 8)
        for mm in (0, 1):
            m = 2 * r + mm
            at = slice(W * mm, W * mm + W)
            gb = gbr[r, :, :, at].astype(f32).reshape(CH, W)
            gp = jnp.concatenate(
                [gb * fac[m, 256:384, :], gb * fac[m, 384:512, :]], axis=0
            ).astype(bf16)
            gps[m, 256:512, :] = gp
            acc_right[...] += dot(nrm[m], gp, 1, 1)
        return 0

    lax.fori_loop(0, CHUNKS, finish, 0)
    p2s[0] = blocks(acc_right[...] * INV)
    send(p2s, p2r, 0, 10)
    sum_both(h1s, h1r, g1s, g1r, 11, 12)

    def last(m, _):
        gn = dot(w_in[...], gps[m], 1, 0) + gate[m]
        zhat, rstd = start[m], scale[m, 0:1, :]
        acc_norm[...] += lane_sum(gn * zhat)
        gz = norm_grad(gn * cols[:, 4:5], zhat, rstd)
        res = (cott[m].astype(f32) + gz).astype(bf16)
        out[pl.ds(2 * m, 2)] = dot(sel[...], res, 1, 1).astype(bf16).reshape(2, RES, CH)
        return 0

    lax.fori_loop(0, CHUNKS, last, 0)
    sum_half(p3r, h3s, h3r, 13, 14)
    lax.fori_loop(CHUNKS, 2 * CHUNKS, last, 0)

    sums[0:1, :] = jnp.sum(acc_norm[...].T, axis=0, keepdims=True)
    g4s[...] = (sums[0:2, :] * INV).astype(bf16)
    share(g4s, g4r, 17)
    wait(p2r, 0, 10)
    g2s[...] = summed(p2r.at[0], DEV).astype(bf16)
    share(g2s, g2r, 16)
    sum_both(h3s, h3r, g3s, g3r, 14, 15)

    for ident, ref in ((12, g1r), (17, g4r), (15, g3r), (16, g2r)):
        got = ref.at[pl.ds(0, ref.shape[0] - 1)]
        pltpu.make_async_copy(got, got, recv_sem.at[ident, 0]).wait()
    o_all[0:CH, 0:256] = g3r[...].astype(f32).reshape(CH, 256)
    o_all[0:CH, 256:512] = g2r[...].astype(f32).reshape(CH, 256)
    o_all[0:CH, 512:768] = g1r[...].astype(f32).reshape(CH, 256)
    o_all[CH : CH + 2, 0:128] = summed(g4r, DEV)

    for ident, ref, rest in (
        (0, b1r, (0, 1, 2)), (1, a1s, (0, 1, 2)), (2, x1s, (0, 1, 2)), (3, b2s, (0,)),
        (4, a2s, (0, 1, 2)), (5, x2s, (0, 1, 2)), (6, gxs, (0, 1, 2)), (7, gas, (0, 1, 2)),
        (8, gbs, (0, 1, 2)),
        (9, p1s, (0,)), (10, p2s, (0,)), (13, p3s, (0,)),
    ):
        for r in rest:
            sent(ref, r, ident)
    for ident, ref in ((12, g1r), (17, g4r), (15, g3r), (16, g2r)):
        gone = ref.at[pl.ds(0, ref.shape[0] - 1)]
        pltpu.make_async_copy(gone, gone, send_sem.at[ident, 0]).wait()
    across(h1s, h1r, 11).wait_send()
    across(h3s, h3r, 14).wait_send()


def deliver(pair_in, all_in, pair_out, proj, gate, final, norm, mid, sem):
    copies = [
        pltpu.make_async_copy(src, dst, sem.at[i])
        for i, (src, dst) in enumerate(
            (
                (pair_in, pair_out),
                (all_in.at[0:CH, 0:512], proj),
                (all_in.at[0:CH, 512:640], gate),
                (all_in.at[0:CH, 640:768], final),
            )
        )
    ]
    for copy in copies:
        copy.start()
    norm[...] = all_in[CH : CH + 1, 0:128]
    mid[...] = all_in[CH + 1 : CH + 2, 0:128]
    for copy in copies:
        copy.wait()


def shards(
    pair, cotangent, residue_mask, chain_ids, chain_embed, out_norm_gain, out_proj, out_gate,
    out_mid_gain, out_final, in_norm_gain, in_proj, in_gate, in_mid_gain, in_final,
):
    vm = pl.BlockSpec(memory_space=pltpu.VMEM)
    hbm = pl.BlockSpec(memory_space=pl.ANY)
    v = pltpu.VMEM
    wire = v((CHUNKS, DEV, CG, LANES), bf16)
    half = v((CHUNKS, HDEV, HG, LANES), bf16)
    twice = v((CHUNKS, DEV, HG, LANES), bf16)
    steps = lambda dtype: v((2 * CHUNKS, CH, W), dtype)
    part, part2 = v((1, HDEV, HG, 256), bf16), v((1, DEV, CG, 256), bf16)
    piece, piece2, row = v((HG, 256), bf16), v((CG, 256), bf16), v((2, CH), bf16)
    full, full2 = v((HDEV, HG, 256), bf16), v((DEV, CG, 256), bf16)
    rows = v((DEV, 2, CH), bf16)
    square = v((CH, CH), bf16)
    block = v((ROWS, RES, CH), bf16)
    scratch = (
        [block, block] + [v((1, RES), jnp.int32)] * 2 + [v((2, CH), f32)] + [v((1, CH), f32)] * 4
        + [v((CH, 512), bf16), square, square, v((CH, 512), bf16), square, square]
        + [pltpu.SMEM((1, RES), jnp.int32)] * 2 + [v((2 * CHUNKS, 4 * CH, W), bf16)]
        + [v((2 * CHUNKS, 4 * CH, W), f32), v((2 * CHUNKS, CG, W), f32), v((CG, CH), f32)]
        + [v((W, W), bf16), v((CH, 128), f32), v((CH, 128), f32)]
        + [v((4 * CH, CH), bf16), square, square, v((4 * CH, CH), bf16), square, square]
        + [steps(f32), steps(f32), steps(bf16), steps(bf16), steps(bf16), steps(bf16)]
        + [half] * 3 + [wire] * 6 + [part, part2, part, piece, piece2, piece, row, piece, piece]
        + [twice, half, half] + [wire] * 6 + [part, part2, part, full, full2, full, rows, piece, piece]
        + [v((LANES // 128, DEV * HG, 128), f32), v((LANES // 128, CH, 128), f32)]
        + [v((HG, 256, 256), bf16)]
        + [v((CHUNKS, CG, RES, 128), bf16), v((CG, RES, 256), bf16), v((CHUNKS, CG, 128, 256), bf16)]
        + [v((CH, 256), f32)] * 2 + [v((CH, CH), f32)] * 4
        + [pltpu.SemaphoreType.DMA((18, CHUNKS))] * 2
        + [pltpu.SemaphoreType.DMA((17,))]
    )
    mask = residue_mask.reshape(1, RES)
    chain = chain_ids.reshape(1, RES)
    gains = [g.reshape(1, CH) for g in (out_norm_gain, out_mid_gain, in_norm_gain, in_mid_gain)]
    outs = [
        jax.ShapeDtypeStruct((ROWS, RES, CH), bf16),
        jax.ShapeDtypeStruct((CH, 512), f32),
        jax.ShapeDtypeStruct((CH, CH), f32),
        jax.ShapeDtypeStruct((CH, CH), f32),
        jax.ShapeDtypeStruct((1, CH), f32),
        jax.ShapeDtypeStruct((1, CH), f32),
    ]
    params = pltpu.CompilerParams(
        vmem_limit_bytes=60 * 1024 * 1024, collective_id=0, has_side_effects=True
    )
    got = pl.pallas_call(
        kernel,
        out_shape=[pltpu.VMEM((ROWS, RES, CH), bf16), pltpu.VMEM((CH + CG, 768), f32)],
        in_specs=[hbm] * 15,
        out_specs=[vm, vm],
        scratch_shapes=scratch,
        compiler_params=params,
    )(
        pair, cotangent, mask, chain, chain_embed, *gains,
        out_proj, out_gate, out_final, in_proj, in_gate, in_final,
    )
    got = [pltpu.with_memory_space_constraint(g, pltpu.VMEM) for g in got]
    got = pl.pallas_call(
        deliver,
        out_shape=outs,
        in_specs=[vm] * 2,
        out_specs=[hbm] * 4 + [vm] * 2,
        scratch_shapes=[pltpu.SemaphoreType.DMA((4,))],
    )(*got)
    return (*got[:4], got[4].reshape(CH), got[5].reshape(CH))


def solution(mesh):
    whole = P()
    placed = (P("dap", "cplx", None), P("dap", "cplx", None), P("cplx"), P("cplx")) + (whole,) * 11
    return jax.shard_map(
        shards,
        mesh=mesh,
        in_specs=placed,
        out_specs=(
            P("dap", "cplx", None),
            P("cplx", None),
            P("cplx", None),
            P("cplx", None),
            P("cplx"),
            P("cplx"),
        ),
        check_vma=False,
    )
```
